32 devices in a mesh: hist: 16 (over z, x, core), orb: 2 (over y).
Axes of the slice: x: 2, y: 2, z: 4, core: 2. Of those that a mesh axis runs over, the one named last changes fastest.
Arguments:
- g_hist: bfloat16 [32, 64, 2048], P('hist', 'orb'), may hold values from -6 to 6
- sigma_hist: bfloat16 [2, 64, 2048], P(None, None, 'hist'), may hold values from -0.125 to 0.125
- diag_inv: float32 [32, 64, 64], P('hist'), may hold values from -0.75 to 0.75
- previous: float32 [2, 32, 64, 64], P(None, 'hist', 'orb'), may hold values from -6 to 6
- block_of_slot: int32 [16], replicated, may hold values from 0 to 15, each once
- front_pos: int32 [2], replicated, may hold values from 16 to 31
Outputs:
- g_row: float32 [2, 32, 64, 64], P(None, 'hist', 'orb')
- sigma_row: float32 [2, 32, 64, 64], P(None, 'hist', 'orb')
The draws below stay inside these ranges and needn't reach their ends.
Inputs may be any that keep to these rules, and one draw needn't show every extreme that they name: `block_of_slot`: every block index appears once.
All inputs are finite; a program needn't handle non-finite values.
Results may differ from the reference program's by a relative error of at most 0.0003.
Values may be sent and summed in bfloat16 or wider, within the bound.
A program may use at most 64 MiB of HBM per device.

```python
import jax
import jax.numpy as jnp
from jax import lax

O = 64
TB = 2
NT = 32
N_HIST = 16


def shard_levels(own_key, dims, split, low, largest):
    level = 1.0
    for axis_at, blocks in split:
        steps = jax.random.uniform(jax.random.fold_in(jax.random.fold_in(own_key, 6), axis_at), (blocks,), jnp.float32, low / len(split), largest / len(split))
        level = level * jnp.repeat(jnp.exp(steps), dims[axis_at] // blocks).reshape((-1,) + (1,) * (len(dims) - 1 - axis_at))
    return level


def noise(own_key, dims, spread, bound, shards=(), held_as=jnp.bfloat16):
    gain = shard_levels(own_key, dims, shards, -0.22, 0.18) if shards else 1.0
    values = jax.random.normal(own_key, dims, jnp.float32) * spread * gain
    return jnp.minimum(jnp.maximum(values, -bound), bound).astype(held_as)


def setup_inputs(seed: int = 0) -> dict:
    key_list = jax.random.split(jax.random.key(seed), 7)
    return {
        "g_hist": noise(key_list[0], (NT, O, NT * O), 1.0, 6.0, ((0, 16), (1, 2))),
        "sigma_hist": noise(key_list[1], (2, O, NT * O), (NT * O) ** -0.5, 0.125, ((2, 16),)),
        "diag_inv": noise(key_list[2], (NT, O, O), O ** -0.5, 0.75, ((0, 16),), jnp.float32),
        "previous": noise(key_list[3], (2, NT, O, O), 1.0, 6.0, ((1, 16), (2, 2)), jnp.float32),
        "block_of_slot": jax.random.permutation(key_list[4], N_HIST).astype(jnp.int32),
        "front_pos": jax.random.randint(key_list[5], (2,), NT // 2, NT).astype(jnp.int32),
    }


COUPLING = 0.5


def reference(g_hist, sigma_hist, diag_inv, previous, block_of_slot, front_pos):
    slot_rows = jnp.arange(NT, dtype=jnp.int32)
    col_time = (block_of_slot[slot_rows // TB] * TB + slot_rows % TB).astype(jnp.int32)
    times = (jnp.arange(NT * O, dtype=jnp.int32) // O).astype(jnp.int32)
    front_keep = times[None, :] <= front_pos[:, None]
    sigma_kept = jnp.where(front_keep[:, None, :], sigma_hist, jnp.zeros_like(sigma_hist)).astype(jnp.float32)

    def column(item):
        g_one, when = item
        g_kept = jnp.where((times >= when)[None, :], g_one, jnp.zeros_like(g_one)).astype(jnp.float32)
        return jnp.einsum("cx,fax->fca", g_kept, sigma_kept)

    integral = lax.map(column, (g_hist, col_time))
    integral = jnp.transpose(integral, (1, 0, 2, 3))
    combined = previous + integral
    rows = diag_inv[front_pos]
    g_row = jnp.einsum("ftcb,fab->ftca", combined, rows, precision=lax.Precision.HIGHEST)
    sigma_row = COUPLING * g_row * g_row * jnp.swapaxes(g_row, 2, 3)
    return g_row, sigma_row
```

```python
import functools

import jax
import jax.numpy as jnp
from jax import lax
from jax.experimental import pallas as pl
from jax.experimental.pallas import tpu as pltpu
from jax.sharding import PartitionSpec as P

COUPLING = 0.5
MESH = pl.DeviceIdType.MESH


def xor(a, b, size):
    out, bit = 0, 1
    while bit < size:
        out = out + bit * ((a // bit + b // bit) % 2)
        bit *= 2
    return out


def loop(low, high, step):
    if high - low <= 8:
        for i in range(low, high):
            step(i)
    else:
        lax.fori_loop(low, high, lambda i, c: (step(i), c)[1], 0)


def split(x):
    high = x.astype(jnp.bfloat16)
    return high, (x - high.astype(jnp.float32)).astype(jnp.bfloat16)


def kernel(lines, blocks_hbm, front_hbm, g_hbm, s_hbm, d_hbm, p_hbm, out,
           blocks, front, g_v, all_s, d_v, p_v, acc, part, total,
           loc, s_send, s_recv, c_send, c_recv, e_send, e_recv, t_send, t_recv,
           y_send, y_recv, ready, s_ready):
    cols, half = g_hbm.shape[0], g_hbm.shape[1]
    fronts, orb, lanes = s_hbm.shape
    me = lax.axis_index("hist")
    o = lax.axis_index("orb")
    core = me % 2
    xi = (me // 2) % 2
    z = me // 4

    def at(zz, xx, cc):
        return (zz * 2 + xx) * 2 + cc

    def scope(name):
        return jax.named_scope(name)

    y_peer = (me, 1 - o)
    core_peer = (at(z, xi, 1 - core), o)
    xc_peer = (at(z, 1 - xi, 1 - core), o)
    near = ((y_peer, o), (core_peer, core), (xc_peer, xi))

    def peer_at(zz, xx):
        return (at(zz, xx, core), o)

    def flip(bit, k):
        return bit + k - 2 * bit * k

    def slot(zz, xx):
        return flip(xi, xx) * lines + xor(zz, z, lines)

    barrier = pltpu.get_barrier_semaphore()

    def signal(sem, peer):
        pl.semaphore_signal(sem, inc=1, device_id=peer, device_id_type=MESH)

    def uppers(step):
        @pl.when(xi == 0)
        def _():
            step(z, 1)

        def one(zz):
            @pl.when(zz > z)
            def _():
                step(zz, 0)
                step(zz, 1)

        loop(1, lines, one)

    def lowers(step):
        def one(zz):
            @pl.when(zz < z)
            def _():
                step(zz, 0)
                step(zz, 1)

        loop(0, lines - 1, one)

        @pl.when(xi == 1)
        def _():
            step(z, 0)

    for peer, upper in near:
        @pl.when(upper == 0)
        def _():
            signal(barrier, peer)

    uppers(lambda zz, xx: signal(barrier, peer_at(zz, xx)))

    load_f = pltpu.make_async_copy(front_hbm, front, loc.at[5])
    load_d = pltpu.make_async_copy(d_hbm, d_v, loc.at[1])
    load_s = pltpu.make_async_copy(s_hbm, all_s.at[z, xi, core], loc.at[0])
    load_g = pltpu.make_async_copy(g_hbm, g_v.at[o], loc.at[2])
    load_p = pltpu.make_async_copy(p_hbm, p_v.at[o], loc.at[3])
    load_b = pltpu.make_async_copy(blocks_hbm, blocks, loc.at[4])
    load_f.start()
    load_d.start()

    below = 2 * z + 2 * xi + core + o
    with scope("Abar"):
        @pl.when(below > 0)
        def _():
            pl.semaphore_wait(barrier, below)

    for k, (peer, upper) in enumerate(near):
        @pl.when(upper == 1)
        def _():
            signal(ready.at[k], peer)

    lowers(lambda zz, xx: signal(s_ready.at[slot(zz, xx)], peer_at(zz, xx)))

    def send(src, dst, ssem, rsem, peer):
        return pltpu.make_async_remote_copy(
            src_ref=src, dst_ref=dst, send_sem=ssem, recv_sem=rsem,
            device_id=peer, device_id_type=MESH)

    def s_copy(zz, xx):
        k = slot(zz, xx)
        return send(s_hbm, all_s.at[z, xi, core], s_send.at[k], s_recv.at[k], peer_at(zz, xx))

    def c_copy(zz, xx, own=False):
        k = slot(zz, xx)
        ref = all_s.at[zz, xx, core]
        return send(s_hbm if own else ref, ref, c_send.at[k], c_recv.at[k], core_peer)

    def t_copy(zz):
        d = xor(zz, z, lines)
        return send(total.at[0], total.at[d], t_send.at[d], t_recv.at[d], peer_at(zz, xi))

    e_copies = [send(part.at[0], part.at[1 + k], e_send.at[k], e_recv.at[k], peer)
                for k, peer in enumerate((peer_at(z, 1 - xi), xc_peer, core_peer))]
    g_copy = send(g_hbm, g_v.at[o], y_send.at[0], y_recv.at[0], y_peer)
    p_copy = send(p_hbm, p_v.at[o], y_send.at[1], y_recv.at[1], y_peer)

    lowers(lambda zz, xx: s_copy(zz, xx).start())

    @pl.when(core == 1)
    def _():
        c_copy(z, xi, True).start()

    @pl.when(o == 1)
    def _():
        g_copy.start()
        p_copy.start()

    load_b.start()
    load_s.start()
    load_g.start()
    load_p.start()

    with scope("Bload"):
        load_f.wait()
        load_d.wait()
    rows = []
    for f in range(fronts):
        row = d_v[front[f] % cols]
        rows.append(jnp.where(front[f] // cols == me, row, jnp.zeros_like(row)))
    part[0] = jnp.concatenate(rows, axis=1)

    @pl.when(xi == 1)
    def _():
        e_copies[0].start()
        e_copies[1].start()

    @pl.when(core == 1)
    def _():
        e_copies[2].start()

    with scope("Cnear"):
        @pl.when(core == 0)
        def _():
            pl.semaphore_wait(ready.at[1], 1)
            e_copies[2].start()
            c_copy(z, xi, True).start()

        @pl.when(o == 0)
        def _():
            pl.semaphore_wait(ready.at[0], 1)
            g_copy.start()
            p_copy.start()

        @pl.when(xi == 0)
        def _():
            pl.semaphore_wait(s_ready.at[slot(z, 1)], 1)
            e_copies[0].start()
            pl.semaphore_wait(ready.at[2], 1)
            e_copies[1].start()
            s_copy(z, 1).start()

    acc[...] = jnp.zeros_like(acc)

    def depart(zz):
        @pl.when(zz > z)
        def _():
            for xx in range(2):
                pl.semaphore_wait(s_ready.at[slot(zz, xx)], 1)
                s_copy(zz, xx).start()

    with scope("Dfar"):
        loop(1, lines, depart)

    with scope("Ediag"):
        for c in e_copies:
            c.wait_recv()
    total[0] = (part[0] + part[1]) + (part[2] + part[3])

    def spread(zz):
        @pl.when(zz != z)
        def _():
            t_copy(zz).start()

    loop(0, lines, spread)

    load_b.wait()
    col0 = blocks[me] * cols
    one, zero = jnp.float32(1), jnp.float32(0)

    def arrive(zz, xx):
        s_copy(zz, xx).wait_recv()
        c_copy(zz, xx).start()

    def product(zz, xx):
        width = 2 * lanes
        start = pl.multiple_of((zz * 2 + xx) * width, width)
        time = (lax.broadcasted_iota(jnp.int32, (1, width), 1) + start) // orb

        def mask(hit):
            return jnp.where(hit, one, zero).astype(jnp.bfloat16)

        left = []
        for t in range(cols):
            keep = mask(time >= col0 + t)
            left += [g_v[h, t, :, pl.ds(start, width)] * keep for h in range(2)]
        right = []
        for f in range(fronts):
            keep = mask(time <= front[f])
            right.append(jnp.concatenate([all_s[zz, xx, 0, f], all_s[zz, xx, 1, f]], axis=1) * keep)
        acc[...] += lax.dot_general(jnp.concatenate(left, axis=0), jnp.concatenate(right, axis=0),
                                    (((1,), (1,)), ((), ())), preferred_element_type=jnp.float32)

    def relay(d):
        zz = xor(z, d, lines)
        with scope("Fz"):
            arrive(zz, xi)
        with scope("Fx"):
            arrive(zz, 1 - xi)

    def use(d):
        zz = xor(z, d, lines)
        c_copy(zz, xi).wait_recv()
        product(zz, xi)
        c_copy(zz, 1 - xi).wait_recv()
        product(zz, 1 - xi)

    with scope("Fx0"):
        arrive(z, 1 - xi)
    loop(1, lines - 1, relay)
    with scope("Gg"):
        load_s.wait()
        load_g.wait()
        g_copy.wait_recv()
    with scope("Huse"):
        loop(0, lines - 2, use)
    with scope("Ilast"):
        loop(lines - 1, lines, relay)
    with scope("Juse"):
        loop(lines - 2, lines, use)

    with jax.named_scope("Kp"):
        load_p.wait()
        p_copy.wait_recv()
    prev = jnp.concatenate(
        [jnp.concatenate([p_v[h, f, t] for f in range(fronts)], axis=1)
         for t in range(cols) for h in range(2)], axis=0)
    combined = acc[...] + prev
    with jax.named_scope("Le"):
        def gather(zz):
            @pl.when(zz != z)
            def _():
                t_copy(zz).wait_recv()

        loop(0, lines, gather)
    both = lax.fori_loop(1, lines, lambda d, v: v + total[d], total[0])
    lane = lax.broadcasted_iota(jnp.int32, both.shape, 1) // orb
    weight = jnp.concatenate([jnp.where(lane == f, both, jnp.zeros_like(both))
                              for f in range(fronts)], axis=0)

    def mine(x):
        blocks_of = [x[k * half:(k + 1) * half] for k in range(x.shape[0] // half)]
        return jnp.concatenate([jnp.where(o == 0, blocks_of[k], blocks_of[k + 1])
                                for k in range(0, len(blocks_of), 2)], axis=0)

    def times(a, b):
        (a0, a1), (b0, b1) = split(a), split(b)
        return lax.dot_general(jnp.concatenate([a0, a1, a0], axis=1), jnp.concatenate([b0, b0, b1], axis=1),
                               (((1,), (1,)), ((), ())), preferred_element_type=jnp.float32)

    g_new = times(mine(combined), weight)
    flipped = times(mine(weight), combined)
    for t in range(cols):
        g_t = g_new[t * half:(t + 1) * half]
        turned = jnp.concatenate([flipped[f * half:(f + 1) * half, t * orb:(t + 1) * orb]
                                  for f in range(fronts)], axis=1)
        s_t = COUPLING * g_t * g_t * turned
        for f in range(fronts):
            out[f, t] = jnp.concatenate([g_t[:, f * orb:(f + 1) * orb], s_t[:, f * orb:(f + 1) * orb]], axis=1)

    with scope("Msend"):
        g_copy.wait_send()
        p_copy.wait_send()
        for c in e_copies:
            c.wait_send()

        def finish(zz):
            @pl.when(zz != z)
            def _():
                t_copy(zz).wait_send()
                s_copy(zz, xi).wait_send()
                s_copy(zz, 1 - xi).wait_send()
                c_copy(zz, xi).wait_send()
                c_copy(zz, 1 - xi).wait_send()

        loop(0, lines, finish)
        s_copy(z, 1 - xi).wait_send()
        c_copy(z, xi, True).wait_send()
        c_copy(z, 1 - xi).wait_send()


def body(lines, g_hist, sigma_hist, diag_inv, previous, block_of_slot, front_pos):
    cols, half, depth = g_hist.shape
    fronts, orb, lanes = sigma_hist.shape
    hbm = pl.BlockSpec(memory_space=pl.ANY)
    dma = pltpu.SemaphoreType.DMA
    regular = pltpu.SemaphoreType.REGULAR
    f32 = jnp.float32
    flops = 2 * cols * orb * depth * orb * fronts
    out = pl.pallas_call(
        functools.partial(kernel, lines),
        out_shape=pltpu.VMEM((fronts, cols, half, 2 * orb), f32),
        in_specs=[hbm] * 6,
        out_specs=pl.BlockSpec(memory_space=pltpu.VMEM),
        scratch_shapes=[
            pltpu.SMEM(block_of_slot.shape, jnp.int32),
            pltpu.SMEM(front_pos.shape, jnp.int32),
            pltpu.VMEM((2,) + g_hist.shape, g_hist.dtype),
            pltpu.VMEM((lines, 2, 2) + sigma_hist.shape, sigma_hist.dtype),
            pltpu.VMEM(diag_inv.shape, f32),
            pltpu.VMEM((2,) + previous.shape, f32),
            pltpu.VMEM((cols * orb, fronts * orb), f32),
            pltpu.VMEM((4, orb, fronts * orb), f32),
            pltpu.VMEM((lines, orb, fronts * orb), f32),
            dma((6,)),
            dma((2 * lines,)), dma((2 * lines,)),
            dma((2 * lines,)), dma((2 * lines,)),
            dma((3,)), dma((3,)),
            dma((lines,)), dma((lines,)),
            dma((2,)), dma((2,)),
            regular((3,)), regular((2 * lines,)),
        ],
        compiler_params=pltpu.CompilerParams(collective_id=0, has_side_effects=True),
        cost_estimate=pl.CostEstimate(flops=flops, bytes_accessed=2 * g_hist.size, transcendentals=0),
    )(block_of_slot, front_pos, g_hist, sigma_hist, diag_inv, previous)
    return out[..., :orb], out[..., orb:]


def solution(mesh):
    lines = mesh.shape["hist"] // 4
    in_specs = (
        P("hist", "orb", None),
        P(None, None, "hist"),
        P("hist", None, None),
        P(None, "hist", "orb", None),
        P(),
        P(),
    )
    out_specs = (P(None, "hist", "orb", None), P(None, "hist", "orb", None))
    return jax.shard_map(functools.partial(body, lines), mesh=mesh, in_specs=in_specs,
                         out_specs=out_specs, check_vma=False)
```

```python
import functools

import jax
import jax.numpy as jnp
from jax import lax
from jax.experimental import pallas as pl
from jax.experimental.pallas import tpu as pltpu
from jax.sharding import PartitionSpec as P

COUPLING = 0.5
MESH = pl.DeviceIdType.MESH


def xor(a, b, size):
    out, bit = 0, 1
    while bit < size:
        out = out + bit * ((a // bit + b // bit) % 2)
        bit *= 2
    return out


def loop(low, high, step):
    if high - low <= 8:
        for i in range(low, high):
            step(i)
    else:
        lax.fori_loop(low, high, lambda i, c: (step(i), c)[1], 0)


def split(x):
    high = x.astype(jnp.bfloat16)
    return high, (x - high.astype(jnp.float32)).astype(jnp.bfloat16)


def kernel(lines, blocks_hbm, front_hbm, g_hbm, s_hbm, d_hbm, p_hbm, out,
           blocks, front, g_v, all_s, d_v, p_v, p_all, acc, col_d, cross_d, sums, sent, sent_rows,
           loc, sends, dc_send, dz_send, x_send, root_send, z_recv, x_recv, c_recv, near_recv, ready):
    cols, half = g_hbm.shape[0], g_hbm.shape[1]
    fronts, orb, lanes = s_hbm.shape
    width = 2 * lanes
    me = lax.axis_index("hist")
    o = lax.axis_index("orb")
    core = me % 2
    xi = (me // 2) % 2
    z = me // 4
    late = lines // 2
    has_rows = z >= late
    first = (z == 0) & (xi == 0)
    beside = (z == 0) & (xi == 1)
    across = (z == lines - 1) & (xi == 1)
    special = jnp.where(z == lines - 1, 0, lines - 1)

    def at(zz, xx, cc):
        return (zz * 2 + xx) * 2 + cc

    def scope(name):
        return jax.named_scope(name)

    y_peer = (me, 1 - o)
    core_peer = (at(z, xi, 1 - core), o)
    x_peer = (at(z, 1 - xi, core), o)
    xc_peer = (at(z, 1 - xi, 1 - core), o)
    near = ((y_peer, o), (core_peer, core), (x_peer, xi), (xc_peer, xi))

    def z_peer(zz):
        return (at(zz, xi, core), o)

    def dist(zz):
        return xor(zz, z, lines)

    barrier = pltpu.get_barrier_semaphore()

    def signal(sem, peer):
        pl.semaphore_signal(sem, inc=1, device_id=peer, device_id_type=MESH)

    def above(step):
        def one(zz):
            @pl.when(zz > z)
            def _():
                step(zz)

        loop(1, lines, one)

    def below(step, low=0):
        def one(zz):
            @pl.when(zz < z)
            def _():
                step(zz)

        loop(low, lines - 1, one)

    for peer, upper in near:
        @pl.when(upper == 0)
        def _():
            signal(barrier, peer)

    above(lambda zz: signal(barrier, z_peer(zz)))

    @pl.when(first)
    def _():
        loop(late, lines, lambda zz: signal(barrier, (at(zz, 1, core), o)))

    load_f = pltpu.make_async_copy(front_hbm, front, loc.at[0])
    load_d = pltpu.make_async_copy(d_hbm, d_v.at[core], loc.at[1])
    load_s = pltpu.make_async_copy(s_hbm, all_s.at[z, xi, core], loc.at[2])
    load_g = pltpu.make_async_copy(g_hbm, g_v.at[o], loc.at[3])
    load_p = pltpu.make_async_copy(p_hbm, p_v, loc.at[4])
    load_b = pltpu.make_async_copy(blocks_hbm, blocks, loc.at[5])
    load_f.start()

    @pl.when(has_rows)
    def _():
        load_d.start()

    earlier = z + 2 * xi + core + o + jnp.where(has_rows, xi, 0)
    with scope("Abar"):
        @pl.when(earlier > 0)
        def _():
            pl.semaphore_wait(barrier, earlier)

    for k, (peer, upper) in enumerate(near):
        @pl.when(upper == 1)
        def _():
            signal(ready.at[k], peer)

    below(lambda zz: signal(ready.at[len(near) + dist(zz) - 1], z_peer(zz)))

    def send(src, dst, rsem, peer, ssem=sends):
        return pltpu.make_async_remote_copy(
            src_ref=src, dst_ref=dst, send_sem=ssem, recv_sem=rsem,
            device_id=peer, device_id_type=MESH)

    def arrived(ref, sem):
        pltpu.make_async_copy(ref, ref, sem).wait()

    def z_copy(zz):
        return send(s_hbm, all_s.at[z, xi, core], z_recv.at[dist(zz) - 1], z_peer(zz))

    def x_copy(zz, own=False, ssem=sends):
        ref = all_s.at[zz, xi, core]
        return send(s_hbm if own else ref, ref, x_recv.at[dist(zz)], x_peer, ssem)

    root_copy = send(s_hbm, all_s.at[z, xi, core], x_recv.at[z], (core, o), root_send)

    def c_copy(zz, xx, own=False):
        ref = all_s.at[zz, xx, core]
        return send(s_hbm if own else ref, ref, c_recv.at[dist(zz)], core_peer)

    def part_of(zz):
        return pl.ds(pl.multiple_of(zz * 2 * width, 2 * width), 2 * width)

    def g_copy(d):
        part = part_of(xor(z, d, lines))
        return send(g_hbm.at[:, :, part], g_v.at[o, :, :, part], near_recv.at[0], y_peer)

    def dz_copy(zz):
        return send(col_d.at[z - late], col_d.at[z - late], near_recv.at[2], z_peer(zz), dz_send)

    droot_copy = send(col_d.at[z - late], cross_d.at[z - late], near_recv.at[5], (core, o), root_send)
    p_copy = send(p_all.at[o], p_all.at[o], near_recv.at[1], y_peer)
    dc_copy = send(d_hbm, d_v.at[core], near_recv.at[4], core_peer, dc_send)
    sum_copies = [send(sums.at[0], sums.at[1 + k], near_recv.at[3], peer, x_send)
                  for k, peer in enumerate((x_peer, xc_peer))]
    core_sum = send(sums.at[4], sums.at[3], near_recv.at[3], core_peer)

    @pl.when(has_rows & (core == 1))
    def _():
        dc_copy.start()

    @pl.when(z == lines - 1)
    def _():
        z_copy(lines - 2).start()
        loop(0, lines - 2, lambda zz: z_copy(zz).start())

        @pl.when(xi == 1)
        def _():
            root_copy.start()

    @pl.when(z < lines - 1)
    def _():
        below(lambda zz: z_copy(zz).start())

    @pl.when(xi == 1)
    def _():
        x_copy(z, True).start()

    @pl.when(core == 1)
    def _():
        c_copy(z, xi, True).start()

    @pl.when(o == 1)
    def _():
        loop(1, lines, lambda d: g_copy(d).start())

    load_s.start()
    load_g.start()
    load_p.start()
    load_b.start()

    @pl.when(core == 0)
    def _():
        with scope("Bcore"):
            pl.semaphore_wait(ready.at[1], 1)

        @pl.when(has_rows)
        def _():
            dc_copy.start()

        c_copy(z, xi, True).start()

    load_f.wait()

    @pl.when(has_rows)
    def _():
        with scope("Bload"):
            load_d.wait()
            dc_copy.wait_recv()
        mine = front[core]
        row = d_v[(mine // cols) % 2, mine % cols]
        row = jnp.where(mine // (2 * cols) == me // 2, row, jnp.zeros_like(row))
        col_d[z - late] = jnp.concatenate([row[:half], row[half:]], axis=1)

        @pl.when(xi == 1)
        def _():
            droot_copy.start()

        below(lambda zz: dz_copy(zz).start())

    with scope("Cnear"):
        @pl.when(o == 0)
        def _():
            pl.semaphore_wait(ready.at[0], 1)
            loop(1, lines, lambda d: g_copy(d).start())

        @pl.when(xi == 0)
        def _():
            pl.semaphore_wait(ready.at[2], 1)
            x_copy(z, True).start()
            pl.semaphore_wait(ready.at[3], 1)

    acc[...] = jnp.zeros_like(acc)

    def depart(zz):
        pl.semaphore_wait(ready.at[len(near) + dist(zz) - 1], 1)
        z_copy(zz).start()

        @pl.when(has_rows)
        def _():
            dz_copy(zz).start()

    with scope("Dfar"):
        above(depart)

    one, zero = jnp.float32(1), jnp.float32(0)

    def mask(hit):
        return jnp.where(hit, one, zero).astype(jnp.bfloat16)

    def product(zz, xx, hs):
        start = pl.multiple_of((zz * 2 + xx) * width, width)
        time = (lax.broadcasted_iota(jnp.int32, (1, width), 1) + start) // orb
        left = []
        for t in range(cols):
            keep = mask(time >= blocks[me] * cols + t)
            left += [g_v[h, t, :, pl.ds(start, width)] * keep for h in hs]
        right = []
        for f in range(fronts):
            keep = mask(time <= front[f])
            right.append(jnp.concatenate([all_s[zz, xx, 0, f], all_s[zz, xx, 1, f]], axis=1) * keep)
        return lax.dot_general(jnp.concatenate(left, axis=0), jnp.concatenate(right, axis=0),
                               (((1,), (1,)), ((), ())), preferred_element_type=jnp.float32)

    def outward(step):
        def both(d):
            @pl.when(z + d < lines)
            def _():
                step(z + d, d)

            @pl.when(z >= d)
            def _():
                step(z - d, d)

        return both

    @outward
    def z_relay(zz, d):
        with scope("Fz"):
            z_copy(zz).wait_recv()
        @pl.when(zz != special)
        def _():
            x_copy(zz).start()

        @pl.when((zz == special) & ~beside)
        def _():
            x_copy(zz, ssem=x_send).start()

        c_copy(zz, xi).start()

    def x_step(zz, d):
        with scope("Gx"):
            x_copy(zz).wait_recv()
        c_copy(zz, 1 - xi).start()

    x_relay = outward(x_step)

    def c_wait(zz):
        arrived(all_s.at[zz, :, 1 - core], c_recv.at[dist(zz)])

    def use(d):
        zz = xor(z, d, lines)
        with scope("Hc"):
            c_wait(zz)
        value = product(zz, xi, range(2)) + product(zz, 1 - xi, range(2))
        acc[...] += value.reshape(acc.shape)

    z_relay(1)
    with scope("Ex0"):
        x_step(z, 0)
    with scope("Eown"):
        load_s.wait()
        load_g.wait()
        load_p.wait()
        load_b.wait()
        c_wait(z)
    start_rows = product(z, xi, (o,)) + product(z, 1 - xi, (o,))
    for t in range(cols):
        prev = jnp.concatenate([p_v[f, t] for f in range(fronts)], axis=1)
        p_all[o, t] = start_rows[t * half:(t + 1) * half] + prev
    p_copy.start()

    loop(2, lines, z_relay)
    x_relay(1)

    with scope("Idz"):
        @pl.when(has_rows)
        def _():
            arrived(col_d.at[pl.ds(0, late - 1)], near_recv.at[2])

        @pl.when(z < late)
        def _():
            arrived(col_d, near_recv.at[2])

    sums[0] = lax.fori_loop(1, late, lambda d, v: v + col_d[d], col_d[0])
    sums[4] = sums[0]

    @pl.when(~beside)
    def _():
        for c in sum_copies:
            c.start()

    @pl.when(first)
    def _():
        arrived(cross_d, near_recv.at[5])
        sums[4] = lax.fori_loop(0, late, lambda d, v: v + cross_d[d], sums[0])
        sums[1] = jnp.zeros_like(sums[1])
        sums[2] = jnp.zeros_like(sums[2])

    core_sum.start()

    loop(2, lines, x_relay)
    with scope("Jg"):
        arrived(g_v.at[1 - o, :, :, pl.ds(0, (lines - 1) * 2 * width)], near_recv.at[0])
    loop(1, lines, use)

    with scope("Kp"):
        p_copy.wait_recv()
    combined = jnp.concatenate([acc[t, h] + p_all[h, t] for t in range(cols) for h in range(2)], axis=0)
    own = jnp.concatenate([acc[t, o] + p_all[o, t] for t in range(cols)], axis=0)
    combined, own = split(combined), split(own)
    with scope("Lw"):
        @pl.when(first)
        def _():
            core_sum.wait_recv()

        @pl.when(~first)
        def _():
            arrived(sums.at[pl.ds(1, 3)], near_recv.at[3])

    same, other = sums[4] + sums[1], sums[3] + sums[2]
    rows = [jnp.where(core == 0, same, other), jnp.where(core == 0, other, same)]
    lane = lax.broadcasted_iota(jnp.int32, (half, fronts * orb), 1) // orb
    blocks_w = []
    for f in range(fronts):
        turned = pltpu.roll(rows[f], orb, 1)
        none = jnp.zeros_like(turned)
        blocks_w.append([jnp.where(lane == f, rows[f] if h == f else turned, none) for h in range(2)])
    weight = split(jnp.concatenate([w for pair in blocks_w for w in pair], axis=0))
    own_weight = split(jnp.concatenate([jnp.where(o == 0, pair[0], pair[1]) for pair in blocks_w], axis=0))

    def times(a, b):
        return lax.dot_general(jnp.concatenate([a[0], a[1], a[0]], axis=1),
                               jnp.concatenate([b[0], b[0], b[1]], axis=1),
                               (((1,), (1,)), ((), ())), preferred_element_type=jnp.float32)

    g_new = times(own, weight)
    flipped = times(own_weight, combined)
    for t in range(cols):
        g_t = g_new[t * half:(t + 1) * half]
        turned = jnp.concatenate([flipped[f * half:(f + 1) * half, t * orb:(t + 1) * orb]
                                  for f in range(fronts)], axis=1)
        s_t = COUPLING * g_t * g_t * turned
        for f in range(fronts):
            out[f, t] = jnp.concatenate([g_t[:, f * orb:(f + 1) * orb], s_t[:, f * orb:(f + 1) * orb]], axis=1)

    with scope("Msend"):
        @pl.when(has_rows)
        def _():
            dc_copy.wait_send()
            arrived(sent_rows, dz_send)

        @pl.when(across)
        def _():
            root_copy.wait_send()

        @pl.when(has_rows & (xi == 1))
        def _():
            droot_copy.wait_send()

        @pl.when(~beside)
        def _():
            arrived(all_s.at[0, 0], x_send)

        arrived(sent, sends)


def body(lines, g_hist, sigma_hist, diag_inv, previous, block_of_slot, front_pos):
    cols, half, depth = g_hist.shape
    fronts, orb, lanes = sigma_hist.shape
    hbm = pl.BlockSpec(memory_space=pl.ANY)
    dma = pltpu.SemaphoreType.DMA
    regular = pltpu.SemaphoreType.REGULAR
    f32 = jnp.float32
    packed = (orb // 2, 2 * orb)
    width = 2 * lanes
    sent = 2 * (4 * lines - 2) * sigma_hist.size + 2 * g_hist.size * (lines - 1) // lines
    sent += 4 * orb * orb + 4 * cols * half * fronts * orb
    flops = 2 * cols * orb * depth * orb * fronts
    out = pl.pallas_call(
        functools.partial(kernel, lines),
        out_shape=pltpu.VMEM((fronts, cols, half, 2 * orb), f32),
        in_specs=[hbm] * 6,
        out_specs=pl.BlockSpec(memory_space=pltpu.VMEM),
        scratch_shapes=[
            pltpu.SMEM(block_of_slot.shape, jnp.int32),
            pltpu.SMEM(front_pos.shape, jnp.int32),
            pltpu.VMEM((2,) + g_hist.shape, g_hist.dtype),
            pltpu.VMEM((lines, 2, 2) + sigma_hist.shape, sigma_hist.dtype),
            pltpu.VMEM((2,) + diag_inv.shape, f32),
            pltpu.VMEM(previous.shape, f32),
            pltpu.VMEM((2, cols, half, fronts * orb), f32),
            pltpu.VMEM((cols, 2, half, fronts * orb), f32),
            pltpu.VMEM((lines // 2,) + packed, f32),
            pltpu.VMEM((lines // 2,) + packed, f32),
            pltpu.VMEM((5,) + packed, f32),
            pltpu.VMEM((sent // width, width // 2), jnp.bfloat16),
            pltpu.VMEM((lines - 1,) + packed, f32),
            dma((6,)), dma, dma, dma, dma, dma,
            dma((lines - 1,)), dma((lines,)), dma((lines,)),
            dma((6,)), regular((3 + lines,)),
        ],
        compiler_params=pltpu.CompilerParams(collective_id=0, has_side_effects=True),
        cost_estimate=pl.CostEstimate(flops=flops, bytes_accessed=2 * g_hist.size, transcendentals=0),
    )(block_of_slot, front_pos, g_hist, sigma_hist, diag_inv, previous)
    return out[..., :orb], out[..., orb:]


def solution(mesh):
    lines = mesh.shape["hist"] // 4
    in_specs = (
        P("hist", "orb", None),
        P(None, None, "hist"),
        P("hist", None, None),
        P(None, "hist", "orb", None),
        P(),
        P(),
    )
    out_specs = (P(None, "hist", "orb", None), P(None, "hist", "orb", None))
    return jax.shard_map(functools.partial(body, lines), mesh=mesh, in_specs=in_specs,
                         out_specs=out_specs, check_vma=False)
```

```python
import functools

import jax
import jax.numpy as jnp
from jax import lax
from jax.experimental import pallas as pl
from jax.experimental.pallas import tpu as pltpu
from jax.sharding import PartitionSpec as P

COUPLING = 0.5
MESH = pl.DeviceIdType.MESH


def xor(a, b, size):
    out, bit = 0, 1
    while bit < size:
        out = out + bit * ((a // bit + b // bit) % 2)
        bit *= 2
    return out


def loop(low, high, step):
    if high - low <= 8:
        for i in range(low, high):
            step(i)
    else:
        lax.fori_loop(low, high, lambda i, c: (step(i), c)[1], 0)


def split(x):
    high = x.astype(jnp.bfloat16)
    return high, (x - high.astype(jnp.float32)).astype(jnp.bfloat16)


def kernel(lines, blocks_hbm, front_hbm, g_hbm, s_hbm, d_hbm, p_hbm, out,
           blocks, front, g_v, all_s, d_v, p_v, p_all, acc, col_d, cross_d, sums, sent, sent_rows,
           loc, sends, z_recv, x_recv, c_recv, near_recv, ready):
    cols, half = g_hbm.shape[0], g_hbm.shape[1]
    fronts, orb, lanes = s_hbm.shape
    width = 2 * lanes
    me = lax.axis_index("hist")
    o = lax.axis_index("orb")
    core = me % 2
    xi = (me // 2) % 2
    z = me // 4
    late = lines // 2
    has_rows = z >= late
    front_plane = o == 0
    first = (z == 0) & (xi == 0) & front_plane
    beside = (z == 0) & (xi == 1) & front_plane
    across = (z == lines - 1) & (xi == 1) & front_plane
    aside = has_rows & (xi == 1) & front_plane
    special = jnp.where(z == lines - 1, 0, lines - 1)

    def at(zz, xx, cc):
        return (zz * 2 + xx) * 2 + cc

    def scope(name):
        return jax.named_scope(name)

    y_peer = (me, 1 - o)
    core_peer = (at(z, xi, 1 - core), o)
    x_peer = (at(z, 1 - xi, core), o)
    xc_peer = (at(z, 1 - xi, 1 - core), o)
    near = ((y_peer, o), (core_peer, core), (x_peer, xi), (xc_peer, xi))

    def z_peer(zz):
        return (at(zz, xi, core), o)

    def dist(zz):
        return xor(zz, z, lines)

    barrier = pltpu.get_barrier_semaphore()

    def signal(sem, peer):
        pl.semaphore_signal(sem, inc=1, device_id=peer, device_id_type=MESH)

    def above(step):
        def one(zz):
            @pl.when(zz > z)
            def _():
                step(zz)

        loop(1, lines, one)

    def below(step, low=0):
        def one(zz):
            @pl.when(zz < z)
            def _():
                step(zz)

        loop(low, lines - 1, one)

    for peer, upper in near:
        @pl.when(upper == 0)
        def _():
            signal(barrier, peer)

    above(lambda zz: signal(barrier, z_peer(zz)))

    @pl.when(first)
    def _():
        loop(late, lines, lambda zz: signal(barrier, (at(zz, 1, core), o)))

    load_f = pltpu.make_async_copy(front_hbm, front, loc.at[0])
    load_d = pltpu.make_async_copy(d_hbm, d_v.at[core], loc.at[1])
    load_s = pltpu.make_async_copy(s_hbm, all_s.at[z, xi, core], loc.at[2])
    load_g = pltpu.make_async_copy(g_hbm, g_v.at[o], loc.at[2])
    load_p = pltpu.make_async_copy(p_hbm, p_v, loc.at[1])
    load_b = pltpu.make_async_copy(blocks_hbm, blocks, loc.at[0])
    load_f.start()

    @pl.when(has_rows)
    def _():
        load_d.start()

    earlier = z + 2 * xi + core + o + jnp.where(aside, 1, 0)
    with scope("Abar"):
        @pl.when(earlier > 0)
        def _():
            pl.semaphore_wait(barrier, earlier)

    for k, (peer, upper) in enumerate(near):
        @pl.when(upper == 1)
        def _():
            signal(ready.at[min(k, 2)], peer)

    below(lambda zz: signal(ready.at[2 + dist(zz)], z_peer(zz)))

    def send(src, dst, rsem, peer):
        return pltpu.make_async_remote_copy(
            src_ref=src, dst_ref=dst, send_sem=sends, recv_sem=rsem,
            device_id=peer, device_id_type=MESH)

    def arrived(ref, sem):
        pltpu.make_async_copy(ref, ref, sem).wait()

    def z_copy(zz):
        return send(s_hbm, all_s.at[z, xi, core], z_recv.at[dist(zz) - 1], z_peer(zz))

    def x_copy(zz, own=False):
        ref = all_s.at[zz, xi, core]
        return send(s_hbm if own else ref, ref, x_recv.at[dist(zz)], x_peer)

    root_copy = send(s_hbm, all_s.at[z, xi, core], x_recv.at[z], (core, o))

    def c_copy(zz, xx, own=False):
        ref = all_s.at[zz, xx, core]
        return send(s_hbm if own else ref, ref, c_recv.at[dist(zz)], core_peer)

    def part_of(zz):
        return pl.ds(pl.multiple_of(zz * 2 * width, 2 * width), 2 * width)

    def g_copy(d):
        part = part_of(xor(z, d, lines))
        return send(g_hbm.at[:, :, part], g_v.at[o, :, :, part], near_recv.at[0], y_peer)

    def dz_copy(zz):
        return send(col_d.at[z - late], col_d.at[z - late], near_recv.at[1], z_peer(zz))

    droot_copy = send(col_d.at[z - late], cross_d.at[z - late], near_recv.at[3], (core, o))
    p_copy = send(p_all.at[o], p_all.at[o], near_recv.at[0], y_peer)
    dc_copy = send(d_hbm, d_v.at[core], near_recv.at[3], core_peer)
    sum_copies = [send(sums.at[0], sums.at[1 + k], near_recv.at[2], peer)
                  for k, peer in enumerate((x_peer, xc_peer))]
    core_sum = send(sums.at[4], sums.at[3], near_recv.at[2], core_peer)

    @pl.when(has_rows & (core == 1))
    def _():
        dc_copy.start()

    @pl.when(z == lines - 1)
    def _():
        z_copy(lines - 2).start()
        loop(0, lines - 2, lambda zz: z_copy(zz).start())

        @pl.when(across)
        def _():
            root_copy.start()

    @pl.when(z < lines - 1)
    def _():
        below(lambda zz: z_copy(zz).start())

    @pl.when(xi == 1)
    def _():
        x_copy(z, True).start()

    @pl.when(core == 1)
    def _():
        c_copy(z, xi, True).start()

    @pl.when(o == 1)
    def _():
        loop(1, lines, lambda d: g_copy(d).start())

    load_s.start()
    load_g.start()

    @pl.when(core == 0)
    def _():
        with scope("Bcore"):
            pl.semaphore_wait(ready.at[1], 1)

        @pl.when(has_rows)
        def _():
            dc_copy.start()

        c_copy(z, xi, True).start()

    load_f.wait()
    load_b.start()

    @pl.when(has_rows)
    def _():
        with scope("Bload"):
            load_d.wait()
            dc_copy.wait_recv()
        rows = []
        for f in range(fronts):
            mine = front[f]
            row = d_v[(mine // cols) % 2, mine % cols, pl.ds(core * half, half)]
            rows.append(jnp.where(mine // (2 * cols) == me // 2, row, jnp.zeros_like(row)))
        col_d[z - late] = jnp.concatenate(rows, axis=1)

        @pl.when(aside)
        def _():
            droot_copy.start()

        below(lambda zz: dz_copy(zz).start())

    load_p.start()
    with scope("Cnear"):
        @pl.when(o == 0)
        def _():
            pl.semaphore_wait(ready.at[0], 1)
            loop(1, lines, lambda d: g_copy(d).start())

        @pl.when(xi == 0)
        def _():
            pl.semaphore_wait(ready.at[2], 2)
            x_copy(z, True).start()

    def depart(zz):
        pl.semaphore_wait(ready.at[2 + dist(zz)], 1)
        z_copy(zz).start()

        @pl.when(has_rows)
        def _():
            dz_copy(zz).start()

    with scope("Dfar"):
        above(depart)

    one, zero = jnp.float32(1), jnp.float32(0)

    def mask(hit):
        return jnp.where(hit, one, zero).astype(jnp.bfloat16)

    def start_of(zz, xx):
        return pl.multiple_of((zz * 2 + xx) * width, width)

    def times_of(zz, xx):
        return (lax.broadcasted_iota(jnp.int32, (1, width), 1) + start_of(zz, xx)) // orb

    def left_of(zz, xx, hs):
        left = []
        for t in range(cols):
            keep = mask(times_of(zz, xx) >= blocks[me] * cols + t)
            left += [g_v[h, t, :, pl.ds(start_of(zz, xx), width)] * keep for h in hs]
        return jnp.concatenate(left, axis=0)

    def right_of(zz, xx):
        right = []
        for f in range(fronts):
            keep = mask(times_of(zz, xx) <= front[f])
            right.append(jnp.concatenate([all_s[zz, xx, 0, f], all_s[zz, xx, 1, f]], axis=1) * keep)
        return jnp.concatenate(right, axis=0)

    def product(left, right):
        return lax.dot_general(left, right, (((1,), (1,)), ((), ())), preferred_element_type=jnp.float32)

    def outward(step):
        def both(d):
            @pl.when(z + d < lines)
            def _():
                step(z + d, d)

            @pl.when(z >= d)
            def _():
                step(z - d, d)

        return both

    @outward
    def z_relay(zz, d):
        with scope("Fz"):
            z_copy(zz).wait_recv()
        @pl.when((zz != special) | ~beside)
        def _():
            x_copy(zz).start()

        c_copy(zz, xi).start()

    def x_step(zz, d):
        with scope("Gx"):
            x_copy(zz).wait_recv()
        c_copy(zz, 1 - xi).start()

    x_relay = outward(x_step)

    def c_wait(zz):
        arrived(all_s.at[zz, :, 1 - core], c_recv.at[dist(zz)])

    def value(d):
        zz = xor(z, d, lines)
        lefts = [left_of(zz, xx, range(2)) for xx in range(2)]
        with scope("Hc"):
            c_wait(zz)
        return product(lefts[0], right_of(zz, 0)) + product(lefts[1], right_of(zz, 1))

    def use(d):
        acc[...] += value(d).reshape(acc.shape)

    z_relay(1)
    with scope("Ex0"):
        x_step(z, 0)
    with scope("Eown"):
        arrived(sent.at[pl.ds(0, 2 * (s_hbm.size + g_hbm.size) // (2 * lanes))], loc.at[2])
        load_p.wait()
        load_b.wait()
        c_wait(z)
    start_rows = product(left_of(z, 0, (o,)), right_of(z, 0)) + product(left_of(z, 1, (o,)), right_of(z, 1))
    for t in range(cols):
        prev = jnp.concatenate([p_v[f, t] for f in range(fronts)], axis=1)
        p_all[o, t] = start_rows[t * half:(t + 1) * half] + prev
    p_copy.start()

    loop(2, lines, z_relay)
    x_relay(1)

    with scope("Idz"):
        @pl.when(has_rows)
        def _():
            arrived(col_d.at[pl.ds(0, late - 1)], near_recv.at[1])

        @pl.when(z < late)
        def _():
            arrived(col_d, near_recv.at[1])

    sums[0] = lax.fori_loop(1, late, lambda d, v: v + col_d[d], col_d[0])
    sums[4] = sums[0]

    @pl.when(~beside)
    def _():
        for c in sum_copies:
            c.start()

    @pl.when(~first)
    def _():
        core_sum.start()


    loop(2, lines, x_relay)

    @pl.when(first)
    def _():
        with scope("Icross"):
            arrived(cross_d, near_recv.at[3])
        sums[4] = lax.fori_loop(0, late, lambda d, v: v + cross_d[d], sums[0])
        sums[1] = jnp.zeros_like(sums[1])
        sums[2] = jnp.zeros_like(sums[2])
        core_sum.start()

    with scope("Jg"):
        far = g_hbm.size * (lines - 1) // lines + 2 * p_all.size // 2
        arrived(sent.at[pl.ds(0, 2 * far // (2 * lanes))], near_recv.at[0])
    for t in range(cols):
        for h in range(2):
            acc[t, h] = p_all[h, t]
    loop(1, lines - 1, use)

    final = value(lines - 1) + acc[...].reshape(cols * orb, fronts * orb)
    combined = [final[t * orb:(t + 1) * orb] for t in range(cols)]
    own = split(jnp.concatenate([jnp.where(o == 0, c[:half], c[half:]) for c in combined], axis=0))
    turns = split(jnp.concatenate([combined[(t + k) % cols] for k in range(fronts) for t in range(cols)], axis=0))
    with scope("Lw"):
        @pl.when(first)
        def _():
            core_sum.wait_recv()

        @pl.when(~first)
        def _():
            arrived(sums.at[pl.ds(1, 3)], near_recv.at[2])

    same, other = sums[4] + sums[1], sums[3] + sums[2]
    rows = [jnp.where(core == 0, same, other), jnp.where(core == 0, other, same)]
    mine = jnp.where(o == 0, rows[0], rows[1])
    lane = lax.broadcasted_iota(jnp.int32, (half, fronts * orb), 1) // orb
    none = jnp.zeros_like(mine)
    weight = split(jnp.concatenate([jnp.where(lane == f, r, none) for f in range(fronts) for r in rows], axis=0))
    own_weight = split(jnp.concatenate([jnp.where(lane == f, mine, none) for f in range(fronts)], axis=0))

    def times(a, b):
        return lax.dot_general(jnp.concatenate([a[0], a[1], a[0]], axis=1),
                               jnp.concatenate([b[0], b[0], b[1]], axis=1),
                               (((1,), (1,)), ((), ())), preferred_element_type=jnp.float32)

    def place(f, t):
        k = (t - f) % fronts
        return slice(k * cols * orb, (k + 1) * cols * orb)

    g_new = times(own, weight)
    flipped = times(own_weight, turns)
    for t in range(cols):
        g_t = g_new[t * half:(t + 1) * half]
        turned = sum(jnp.where(lane == f, flipped[f * half:(f + 1) * half, place(f, t)], none) for f in range(fronts))
        s_t = COUPLING * g_t * g_t * turned
        out[0, t] = g_t
        out[1, t] = s_t

    with scope("Msend"):
        @pl.when(has_rows)
        def _():
            dc_copy.wait_send()
            arrived(sent_rows, sends)

        @pl.when(across)
        def _():
            root_copy.wait_send()

        @pl.when(aside)
        def _():
            droot_copy.wait_send()

        @pl.when(~beside)
        def _():
            arrived(all_s.at[0, 0], sends)

        arrived(sent, sends)


def body(lines, g_hist, sigma_hist, diag_inv, previous, block_of_slot, front_pos):
    cols, half, depth = g_hist.shape
    fronts, orb, lanes = sigma_hist.shape
    hbm = pl.BlockSpec(memory_space=pl.ANY)
    dma = pltpu.SemaphoreType.DMA
    regular = pltpu.SemaphoreType.REGULAR
    f32 = jnp.float32
    packed = (orb // 2, 2 * orb)
    width = 2 * lanes
    sent = 2 * (4 * lines - 2) * sigma_hist.size + 2 * g_hist.size * (lines - 1) // lines
    sent += 4 * orb * orb + 4 * cols * half * fronts * orb
    flops = 2 * cols * orb * depth * orb * fronts
    out = pl.pallas_call(
        functools.partial(kernel, lines),
        out_shape=pltpu.VMEM((fronts, cols, half, 2 * orb), f32),
        in_specs=[hbm] * 6,
        out_specs=pl.BlockSpec(memory_space=pltpu.VMEM),
        scratch_shapes=[
            pltpu.SMEM(block_of_slot.shape, jnp.int32),
            pltpu.SMEM(front_pos.shape, jnp.int32),
            pltpu.VMEM((2,) + g_hist.shape, g_hist.dtype),
            pltpu.VMEM((lines, 2, 2) + sigma_hist.shape, sigma_hist.dtype),
            pltpu.VMEM((2,) + diag_inv.shape, f32),
            pltpu.VMEM(previous.shape, f32),
            pltpu.VMEM((2, cols, half, fronts * orb), f32),
            pltpu.VMEM((cols, 2, half, fronts * orb), f32),
            pltpu.VMEM((lines // 2,) + packed, f32),
            pltpu.VMEM((lines // 2,) + packed, f32),
            pltpu.VMEM((5,) + packed, f32),
            pltpu.VMEM((sent // width, width // 2), jnp.bfloat16),
            pltpu.VMEM((lines - 1,) + packed, f32),
            dma((3,)), dma,
            dma((lines - 1,)), dma((lines,)), dma((lines,)),
            dma((4,)), regular((2 + lines,)),
        ],
        compiler_params=pltpu.CompilerParams(collective_id=0, has_side_effects=True),
        cost_estimate=pl.CostEstimate(flops=flops, bytes_accessed=2 * g_hist.size, transcendentals=0),
    )(block_of_slot, front_pos, g_hist, sigma_hist, diag_inv, previous)
    return tuple(jnp.stack([out[k, ..., f * orb:(f + 1) * orb] for f in range(fronts)]) for k in range(2))


def solution(mesh):
    lines = mesh.shape["hist"] // 4
    in_specs = (
        P("hist", "orb", None),
        P(None, None, "hist"),
        P("hist", None, None),
        P(None, "hist", "orb", None),
        P(),
        P(),
    )
    out_specs = (P(None, "hist", "orb", None), P(None, "hist", "orb", None))
    return jax.shard_map(functools.partial(body, lines), mesh=mesh, in_specs=in_specs,
                         out_specs=out_specs, check_vma=False)
```

```python
import functools

import jax
import jax.numpy as jnp
from jax import lax
from jax.experimental import pallas as pl
from jax.experimental.pallas import tpu as pltpu
from jax.sharding import PartitionSpec as P

COUPLING = 0.5
MESH = pl.DeviceIdType.MESH


def xor(a, b, size):
    out, bit = 0, 1
    while bit < size:
        out = out + bit * ((a // bit + b // bit) % 2)
        bit *= 2
    return out


def loop(low, high, step):
    if high - low <= 8:
        for i in range(low, high):
            step(i)
    else:
        lax.fori_loop(low, high, lambda i, c: (step(i), c)[1], 0)


def split(x):
    high = x.astype(jnp.bfloat16)
    return high, (x - high.astype(jnp.float32)).astype(jnp.bfloat16)


def kernel(lines, blocks_hbm, front_hbm, g_hbm, s_hbm, d_hbm, p_hbm, out,
           blocks, front, g_v, all_s, d_v, p_v, p_all, acc, col_d, cross_d, sums, sent, sent_rows,
           loc, sends, z_recv, x_recv, c_recv, near_recv, ready):
    cols, half = g_hbm.shape[0], g_hbm.shape[1]
    fronts, orb, lanes = s_hbm.shape
    width = 2 * lanes
    me = lax.axis_index("hist")
    o = lax.axis_index("orb")
    core = me % 2
    xi = (me // 2) % 2
    z = me // 4
    late = lines // 2
    has_rows = z >= late
    front_plane = o == 0
    first = (z == 0) & (xi == 0) & front_plane
    beside = (z == 0) & (xi == 1) & front_plane
    across = (z == lines - 1) & (xi == 1) & front_plane
    aside = has_rows & (xi == 1) & front_plane
    special = jnp.where(z == lines - 1, 0, lines - 1)

    def at(zz, xx, cc):
        return (zz * 2 + xx) * 2 + cc

    def scope(name):
        return jax.named_scope(name)

    y_peer = (me, 1 - o)
    core_peer = (at(z, xi, 1 - core), o)
    x_peer = (at(z, 1 - xi, core), o)
    xc_peer = (at(z, 1 - xi, 1 - core), o)
    near = ((y_peer, o), (core_peer, core), (x_peer, xi), (xc_peer, xi))

    def z_peer(zz):
        return (at(zz, xi, core), o)

    def dist(zz):
        return xor(zz, z, lines)

    barrier = pltpu.get_barrier_semaphore()

    def signal(sem, peer):
        pl.semaphore_signal(sem, inc=1, device_id=peer, device_id_type=MESH)

    def above(step):
        def one(zz):
            @pl.when(zz > z)
            def _():
                step(zz)

        loop(1, lines, one)

    def below(step, low=0):
        def one(zz):
            @pl.when(zz < z)
            def _():
                step(zz)

        loop(low, lines - 1, one)

    above(lambda zz: signal(barrier, z_peer(zz)))

    for peer, upper in near:
        @pl.when(upper == 0)
        def _():
            signal(barrier, peer)

    @pl.when(first)
    def _():
        loop(late, lines, lambda zz: signal(barrier, (at(zz, 1, core), o)))

    load_f = pltpu.make_async_copy(front_hbm, front, loc.at[0])
    load_d = pltpu.make_async_copy(d_hbm, d_v.at[core], loc.at[1])
    load_s = pltpu.make_async_copy(s_hbm, all_s.at[z, xi, core], loc.at[2])
    load_g = pltpu.make_async_copy(g_hbm, g_v.at[o], loc.at[2])
    load_p = pltpu.make_async_copy(p_hbm, p_v, loc.at[1])
    load_b = pltpu.make_async_copy(blocks_hbm, blocks, loc.at[0])
    load_f.start()

    @pl.when(has_rows)
    def _():
        load_d.start()

    earlier = z + 2 * xi + core + o + jnp.where(aside, 1, 0)
    with scope("Abar"):
        @pl.when(earlier > 0)
        def _():
            pl.semaphore_wait(barrier, earlier)

    def send(src, dst, rsem, peer):
        return pltpu.make_async_remote_copy(
            src_ref=src, dst_ref=dst, send_sem=sends, recv_sem=rsem,
            device_id=peer, device_id_type=MESH)

    def arrived(ref, sem):
        pltpu.make_async_copy(ref, ref, sem).wait()

    def z_copy(zz):
        return send(s_hbm, all_s.at[z, xi, core], z_recv.at[dist(zz) - 1], z_peer(zz))

    def x_copy(zz, own=False):
        ref = all_s.at[zz, xi, core]
        return send(s_hbm if own else ref, ref, x_recv.at[dist(zz)], x_peer)

    root_copy = send(s_hbm, all_s.at[z, xi, core], x_recv.at[z], (core, o))

    def c_copy(zz, xx, own=False):
        ref = all_s.at[zz, xx, core]
        return send(s_hbm if own else ref, ref, c_recv.at[dist(zz)], core_peer)

    def part_of(zz):
        return pl.ds(pl.multiple_of(zz * 2 * width, 2 * width), 2 * width)

    def g_copy(d):
        part = part_of(xor(z, d, lines))
        return send(g_hbm.at[:, :, part], g_v.at[o, :, :, part], near_recv.at[0], y_peer)

    def dz_copy(zz):
        return send(col_d.at[z - late], col_d.at[z - late], near_recv.at[1], z_peer(zz))

    droot_copy = send(col_d.at[z - late], cross_d.at[z - late], near_recv.at[3], (core, o))
    p_copy = send(p_all.at[o], p_all.at[o], near_recv.at[0], y_peer)
    dc_copy = send(d_hbm, d_v.at[core], near_recv.at[3], core_peer)
    sum_copies = [send(sums.at[0], sums.at[1 + k], near_recv.at[2], peer)
                  for k, peer in enumerate((x_peer, xc_peer))]
    core_sum = send(sums.at[4], sums.at[3], near_recv.at[2], core_peer)

    @pl.when(has_rows & (core == 1))
    def _():
        dc_copy.start()

    @pl.when(z == lines - 1)
    def _():
        z_copy(lines - 2).start()
        loop(0, lines - 2, lambda zz: z_copy(zz).start())

        @pl.when(across)
        def _():
            root_copy.start()

    @pl.when(z < lines - 1)
    def _():
        below(lambda zz: z_copy(zz).start())

    for k, (peer, upper) in enumerate(near):
        @pl.when(upper == 1)
        def _():
            signal(ready.at[min(k, 2)], peer)

    below(lambda zz: signal(ready.at[2 + dist(zz)], z_peer(zz)))

    @pl.when(xi == 1)
    def _():
        x_copy(z, True).start()

    @pl.when(core == 1)
    def _():
        c_copy(z, xi, True).start()

    @pl.when(o == 1)
    def _():
        loop(1, lines, lambda d: g_copy(d).start())

    load_s.start()
    load_g.start()

    @pl.when(core == 0)
    def _():
        with scope("Bcore"):
            pl.semaphore_wait(ready.at[1], 1)

        @pl.when(has_rows)
        def _():
            dc_copy.start()

        c_copy(z, xi, True).start()

    load_f.wait()
    load_b.start()

    @pl.when(has_rows)
    def _():
        with scope("Bload"):
            load_d.wait()
            dc_copy.wait_recv()
        rows = []
        for f in range(fronts):
            mine = front[f]
            row = d_v[(mine // cols) % 2, mine % cols, pl.ds(core * half, half)]
            rows.append(jnp.where(mine // (2 * cols) == me // 2, row, jnp.zeros_like(row)))
        col_d[z - late] = jnp.concatenate(rows, axis=1)

        @pl.when(aside)
        def _():
            droot_copy.start()

        below(lambda zz: dz_copy(zz).start())

    load_p.start()
    with scope("Cnear"):
        @pl.when(o == 0)
        def _():
            pl.semaphore_wait(ready.at[0], 1)
            loop(1, lines, lambda d: g_copy(d).start())

        @pl.when(xi == 0)
        def _():
            pl.semaphore_wait(ready.at[2], 2)
            x_copy(z, True).start()

    def depart(zz):
        pl.semaphore_wait(ready.at[2 + dist(zz)], 1)
        z_copy(zz).start()

        @pl.when(has_rows)
        def _():
            dz_copy(zz).start()

    with scope("Dfar"):
        above(depart)

    one, zero = jnp.float32(1), jnp.float32(0)

    def mask(hit):
        return jnp.where(hit, one, zero).astype(jnp.bfloat16)

    def start_of(zz, xx):
        return pl.multiple_of((zz * 2 + xx) * width, width)

    def times_of(zz, xx):
        return (lax.broadcasted_iota(jnp.int32, (1, width), 1) + start_of(zz, xx)) // orb

    def left_of(zz, xx, hs):
        left = []
        for t in range(cols):
            keep = mask(times_of(zz, xx) >= blocks[me] * cols + t)
            left += [g_v[h, t, :, pl.ds(start_of(zz, xx), width)] * keep for h in hs]
        return jnp.concatenate(left, axis=0)

    def right_of(zz, xx):
        right = []
        for f in range(fronts):
            keep = mask(times_of(zz, xx) <= front[f])
            right.append(jnp.concatenate([all_s[zz, xx, 0, f], all_s[zz, xx, 1, f]], axis=1) * keep)
        return jnp.concatenate(right, axis=0)

    def product(left, right):
        return lax.dot_general(left, right, (((1,), (1,)), ((), ())), preferred_element_type=jnp.float32)

    def outward(step):
        def both(d):
            @pl.when(z + d < lines)
            def _():
                step(z + d, d)

            @pl.when(z >= d)
            def _():
                step(z - d, d)

        return both

    @outward
    def z_relay(zz, d):
        with scope("Fz"):
            z_copy(zz).wait_recv()
        @pl.when((zz != special) | ~beside)
        def _():
            x_copy(zz).start()

        c_copy(zz, xi).start()

    def x_step(zz, d):
        with scope("Gx"):
            x_copy(zz).wait_recv()
        c_copy(zz, 1 - xi).start()

    x_relay = outward(x_step)

    def c_wait(zz):
        arrived(all_s.at[zz, :, 1 - core], c_recv.at[dist(zz)])

    def value(d):
        zz = xor(z, d, lines)
        lefts = [left_of(zz, xx, range(2)) for xx in range(2)]
        with scope("Hc"):
            c_wait(zz)
        return product(jnp.concatenate(lefts, axis=1), jnp.concatenate([right_of(zz, 0), right_of(zz, 1)], axis=1))

    def use(d):
        acc[...] += value(d).reshape(acc.shape)

    z_relay(1)
    with scope("Ex0"):
        x_step(z, 0)
    loop(2, 3, z_relay)
    with scope("Eown"):
        arrived(sent.at[pl.ds(0, 2 * (s_hbm.size + g_hbm.size) // (2 * lanes))], loc.at[2])
        load_p.wait()
        load_b.wait()
        c_wait(z)
    start_rows = product(left_of(z, 0, (o,)), right_of(z, 0)) + product(left_of(z, 1, (o,)), right_of(z, 1))
    for t in range(cols):
        prev = jnp.concatenate([p_v[f, t] for f in range(fronts)], axis=1)
        p_all[o, t] = start_rows[t * half:(t + 1) * half] + prev
    p_copy.start()

    loop(3, lines, z_relay)
    x_relay(1)

    with scope("Idz"):
        @pl.when(has_rows)
        def _():
            arrived(col_d.at[pl.ds(0, late - 1)], near_recv.at[1])

        @pl.when(z < late)
        def _():
            arrived(col_d, near_recv.at[1])

    sums[0] = lax.fori_loop(1, late, lambda d, v: v + col_d[d], col_d[0])
    sums[4] = sums[0]

    @pl.when(~beside)
    def _():
        for c in sum_copies:
            c.start()

    @pl.when(~first)
    def _():
        core_sum.start()


    loop(2, lines, x_relay)

    @pl.when(first)
    def _():
        with scope("Icross"):
            arrived(cross_d, near_recv.at[3])
        sums[4] = lax.fori_loop(0, late, lambda d, v: v + cross_d[d], sums[0])
        sums[1] = jnp.zeros_like(sums[1])
        sums[2] = jnp.zeros_like(sums[2])
        core_sum.start()

    with scope("Jg"):
        far = g_hbm.size * (lines - 1) // lines + 2 * p_all.size // 2
        arrived(sent.at[pl.ds(0, 2 * far // (2 * lanes))], near_recv.at[0])
    for t in range(cols):
        for h in range(2):
            acc[t, h] = p_all[h, t]
    loop(1, lines - 1, use)

    final = value(lines - 1) + acc[...].reshape(cols * orb, fronts * orb)
    combined = [final[t * orb:(t + 1) * orb] for t in range(cols)]
    own = split(jnp.concatenate([jnp.where(o == 0, c[:half], c[half:]) for c in combined], axis=0))
    turns = split(jnp.concatenate([combined[(t + k) % cols] for k in range(fronts) for t in range(cols)], axis=0))
    with scope("Lw"):
        @pl.when(first)
        def _():
            core_sum.wait_recv()

        @pl.when(~first)
        def _():
            arrived(sums.at[pl.ds(1, 3)], near_recv.at[2])

    same, other = sums[4] + sums[1], sums[3] + sums[2]
    rows = [jnp.where(core == 0, same, other), jnp.where(core == 0, other, same)]
    mine = jnp.where(o == 0, rows[0], rows[1])
    lane = lax.broadcasted_iota(jnp.int32, (half, fronts * orb), 1) // orb
    none = jnp.zeros_like(mine)
    weight = split(jnp.concatenate([jnp.where(lane == f, r, none) for f in range(fronts) for r in rows], axis=0))
    own_weight = split(jnp.concatenate([jnp.where(lane == f, mine, none) for f in range(fronts)], axis=0))

    def times(a, b):
        return lax.dot_general(jnp.concatenate([a[0], a[1], a[0]], axis=1),
                               jnp.concatenate([b[0], b[0], b[1]], axis=1),
                               (((1,), (1,)), ((), ())), preferred_element_type=jnp.float32)

    def place(f, t):
        k = (t - f) % fronts
        return slice(k * cols * orb, (k + 1) * cols * orb)

    g_new = times(own, weight)
    flipped = times(own_weight, turns)
    for t in range(cols):
        g_t = g_new[t * half:(t + 1) * half]
        turned = sum(jnp.where(lane == f, flipped[f * half:(f + 1) * half, place(f, t)], none) for f in range(fronts))
        s_t = COUPLING * g_t * g_t * turned
        out[0, t] = g_t
        out[1, t] = s_t

    with scope("Msend"):
        @pl.when(has_rows)
        def _():
            dc_copy.wait_send()
            arrived(sent_rows, sends)

        @pl.when(across)
        def _():
            root_copy.wait_send()

        @pl.when(aside)
        def _():
            droot_copy.wait_send()

        @pl.when(~beside)
        def _():
            arrived(all_s.at[0, 0], sends)

        arrived(sent, sends)


def body(lines, g_hist, sigma_hist, diag_inv, previous, block_of_slot, front_pos):
    cols, half, depth = g_hist.shape
    fronts, orb, lanes = sigma_hist.shape
    hbm = pl.BlockSpec(memory_space=pl.ANY)
    dma = pltpu.SemaphoreType.DMA
    regular = pltpu.SemaphoreType.REGULAR
    f32 = jnp.float32
    packed = (orb // 2, 2 * orb)
    width = 2 * lanes
    sent = 2 * (4 * lines - 2) * sigma_hist.size + 2 * g_hist.size * (lines - 1) // lines
    sent += 4 * orb * orb + 4 * cols * half * fronts * orb
    flops = 2 * cols * orb * depth * orb * fronts
    out = pl.pallas_call(
        functools.partial(kernel, lines),
        out_shape=pltpu.VMEM((fronts, cols, half, 2 * orb), f32),
        in_specs=[hbm] * 6,
        out_specs=pl.BlockSpec(memory_space=pltpu.VMEM),
        scratch_shapes=[
            pltpu.SMEM(block_of_slot.shape, jnp.int32),
            pltpu.SMEM(front_pos.shape, jnp.int32),
            pltpu.VMEM((2,) + g_hist.shape, g_hist.dtype),
            pltpu.VMEM((lines, 2, 2) + sigma_hist.shape, sigma_hist.dtype),
            pltpu.VMEM((2,) + diag_inv.shape, f32),
            pltpu.VMEM(previous.shape, f32),
            pltpu.VMEM((2, cols, half, fronts * orb), f32),
            pltpu.VMEM((cols, 2, half, fronts * orb), f32),
            pltpu.VMEM((lines // 2,) + packed, f32),
            pltpu.VMEM((lines // 2,) + packed, f32),
            pltpu.VMEM((5,) + packed, f32),
            pltpu.VMEM((sent // width, width // 2), jnp.bfloat16),
            pltpu.VMEM((lines - 1,) + packed, f32),
            dma((3,)), dma,
            dma((lines - 1,)), dma((lines,)), dma((lines,)),
            dma((4,)), regular((2 + lines,)),
        ],
        compiler_params=pltpu.CompilerParams(collective_id=0, has_side_effects=True),
        cost_estimate=pl.CostEstimate(flops=flops, bytes_accessed=2 * g_hist.size, transcendentals=0),
    )(block_of_slot, front_pos, g_hist, sigma_hist, diag_inv, previous)
    return tuple(jnp.stack([out[k, ..., f * orb:(f + 1) * orb] for f in range(fronts)]) for k in range(2))


def solution(mesh):
    lines = mesh.shape["hist"] // 4
    in_specs = (
        P("hist", "orb", None),
        P(None, None, "hist"),
        P("hist", None, None),
        P(None, "hist", "orb", None),
        P(),
        P(),
    )
    out_specs = (P(None, "hist", "orb", None), P(None, "hist", "orb", None))
    return jax.shard_map(functools.partial(body, lines), mesh=mesh, in_specs=in_specs,
                         out_specs=out_specs, check_vma=False)
```

```python
import functools

import jax
import jax.numpy as jnp
from jax import lax
from jax.experimental import pallas as pl
from jax.experimental.pallas import tpu as pltpu
from jax.sharding import PartitionSpec as P

COUPLING = 0.5
MESH = pl.DeviceIdType.MESH


def xor(a, b, size):
    out, bit = 0, 1
    while bit < size:
        out = out + bit * ((a // bit + b // bit) % 2)
        bit *= 2
    return out


def loop(low, high, step):
    if high - low <= 8:
        for i in range(low, high):
            step(i)
    else:
        lax.fori_loop(low, high, lambda i, c: (step(i), c)[1], 0)


def split(x):
    high = x.astype(jnp.bfloat16)
    return high, (x - high.astype(jnp.float32)).astype(jnp.bfloat16)


def kernel(lines, blocks_hbm, front_hbm, g_hbm, s_hbm, d_hbm, p_hbm, out,
           blocks, front, g_v, all_s, d_v, p_v, p_all, acc, col_d, cross_d, sums, sent, sent_rows,
           loc, sends, z_recv, x_recv, c_recv, near_recv, ready):
    cols, half = g_hbm.shape[0], g_hbm.shape[1]
    fronts, orb, lanes = s_hbm.shape
    width = 2 * lanes
    me = lax.axis_index("hist")
    o = lax.axis_index("orb")
    core = me % 2
    xi = (me // 2) % 2
    z = me // 4
    late = lines // 2
    has_rows = z >= late
    front_plane = o == 0
    first = (z == 0) & (xi == 0) & front_plane
    beside = (z == 0) & (xi == 1) & front_plane
    direct = front_plane & (core == 0)
    across = (z == lines - 1) & (xi == 1) & direct
    turns_in = (z == lines - 1) & (xi == 0)
    skips = (z < late) & (xi == 1)
    aside = has_rows & (xi == 1) & front_plane
    special = jnp.where(z == lines - 1, 0, lines - 1)

    def at(zz, xx, cc):
        return (zz * 2 + xx) * 2 + cc

    def scope(name):
        return jax.named_scope(name)

    y_peer = (me, 1 - o)
    core_peer = (at(z, xi, 1 - core), o)
    x_peer = (at(z, 1 - xi, core), o)
    xc_peer = (at(z, 1 - xi, 1 - core), o)
    near = ((y_peer, o), (core_peer, core), (x_peer, xi), (xc_peer, xi))

    def z_peer(zz):
        return (at(zz, xi, core), o)

    def dist(zz):
        return xor(zz, z, lines)

    barrier = pltpu.get_barrier_semaphore()

    def signal(sem, peer):
        pl.semaphore_signal(sem, inc=1, device_id=peer, device_id_type=MESH)

    def above(step):
        def one(zz):
            @pl.when(zz > z)
            def _():
                step(zz)

        loop(1, lines, one)

    def below(step, low=0):
        def one(zz):
            @pl.when(zz < z)
            def _():
                step(zz)

        loop(low, lines - 1, one)

    above(lambda zz: signal(barrier, z_peer(zz)))

    for peer, upper in near:
        @pl.when(upper == 0)
        def _():
            signal(barrier, peer)

    @pl.when(first)
    def _():
        loop(late, lines, lambda zz: signal(barrier, (at(zz, 1, core), o)))

    load_f = pltpu.make_async_copy(front_hbm, front, loc.at[0])
    load_d = pltpu.make_async_copy(d_hbm, d_v.at[core], loc.at[1])
    load_s = pltpu.make_async_copy(s_hbm, all_s.at[z, xi, core], loc.at[2])
    load_g = pltpu.make_async_copy(g_hbm, g_v.at[o], loc.at[2])
    load_p = pltpu.make_async_copy(p_hbm, p_v, loc.at[1])
    load_b = pltpu.make_async_copy(blocks_hbm, blocks, loc.at[0])
    load_f.start()

    @pl.when(has_rows)
    def _():
        load_d.start()

    earlier = z + 2 * xi + core + o + jnp.where(aside, 1, 0)
    with scope("Abar"):
        @pl.when(earlier > 0)
        def _():
            pl.semaphore_wait(barrier, earlier)

    def send(src, dst, rsem, peer):
        return pltpu.make_async_remote_copy(
            src_ref=src, dst_ref=dst, send_sem=sends, recv_sem=rsem,
            device_id=peer, device_id_type=MESH)

    def arrived(ref, sem):
        pltpu.make_async_copy(ref, ref, sem).wait()

    def z_copy(zz):
        return send(s_hbm, all_s.at[z, xi, core], z_recv.at[dist(zz) - 1], z_peer(zz))

    def x_copy(zz, own=False):
        ref = all_s.at[zz, xi, core]
        return send(s_hbm if own else ref, ref, x_recv.at[dist(zz)], x_peer)

    root_copy = send(s_hbm, all_s.at[z, xi, core], x_recv.at[z], (core, o))

    def turn_copy(zz):
        ref = all_s.at[lines - 1, 1, core]
        return send(ref, ref, x_recv.at[xor(zz, lines - 1, lines)], z_peer(zz))


    def c_copy(zz, xx, own=False):
        ref = all_s.at[zz, xx, core]
        return send(s_hbm if own else ref, ref, c_recv.at[dist(zz)], core_peer)

    def part_of(zz):
        return pl.ds(pl.multiple_of(zz * 2 * width, 2 * width), 2 * width)

    def g_copy(d):
        part = part_of(xor(z, d, lines))
        return send(g_hbm.at[:, :, part], g_v.at[o, :, :, part], near_recv.at[0], y_peer)

    def dz_copy(zz):
        return send(col_d.at[z - late], col_d.at[z - late], near_recv.at[1], z_peer(zz))

    droot_copy = send(col_d.at[z - late], cross_d.at[z - late], near_recv.at[3], (core, o))
    p_copy = send(p_all.at[o], p_all.at[o], near_recv.at[0], y_peer)
    dc_copy = send(d_hbm, d_v.at[core], near_recv.at[3], core_peer)
    sum_copies = [send(sums.at[0], sums.at[1 + k], near_recv.at[2], peer)
                  for k, peer in enumerate((x_peer, xc_peer))]
    core_sum = send(sums.at[4], sums.at[3], near_recv.at[2], core_peer)

    @pl.when(has_rows & (core == 1))
    def _():
        dc_copy.start()

    @pl.when(z == lines - 1)
    def _():
        z_copy(lines - 2).start()
        loop(0, lines - 2, lambda zz: z_copy(zz).start())

        @pl.when(across)
        def _():
            root_copy.start()

    @pl.when(z < lines - 1)
    def _():
        below(lambda zz: z_copy(zz).start())

    for k, (peer, upper) in enumerate(near):
        @pl.when(upper == 1)
        def _():
            signal(ready.at[min(k, 2)], peer)

    below(lambda zz: signal(ready.at[2 + dist(zz)], z_peer(zz)))

    @pl.when(xi == 1)
    def _():
        x_copy(z, True).start()

    @pl.when(core == 1)
    def _():
        c_copy(z, xi, True).start()

    @pl.when(o == 1)
    def _():
        loop(1, lines, lambda d: g_copy(d).start())

    load_s.start()
    load_g.start()

    @pl.when(core == 0)
    def _():
        with scope("Bcore"):
            pl.semaphore_wait(ready.at[1], 1)

        @pl.when(has_rows)
        def _():
            dc_copy.start()

        c_copy(z, xi, True).start()

    load_f.wait()
    load_b.start()

    @pl.when(has_rows)
    def _():
        with scope("Bload"):
            load_d.wait()
            dc_copy.wait_recv()
        rows = []
        for f in range(fronts):
            mine = front[f]
            row = d_v[(mine // cols) % 2, mine % cols, pl.ds(core * half, half)]
            rows.append(jnp.where(mine // (2 * cols) == me // 2, row, jnp.zeros_like(row)))
        col_d[z - late] = jnp.concatenate(rows, axis=1)

        @pl.when(aside)
        def _():
            droot_copy.start()

        below(lambda zz: dz_copy(zz).start())

    load_p.start()
    with scope("Cnear"):
        @pl.when(o == 0)
        def _():
            pl.semaphore_wait(ready.at[0], 1)
            loop(1, lines, lambda d: g_copy(d).start())

        @pl.when(xi == 0)
        def _():
            pl.semaphore_wait(ready.at[2], 2)
            x_copy(z, True).start()

    def depart(zz):
        pl.semaphore_wait(ready.at[2 + dist(zz)], 1)
        z_copy(zz).start()

        @pl.when(has_rows)
        def _():
            dz_copy(zz).start()

    with scope("Dfar"):
        above(depart)

    one, zero = jnp.float32(1), jnp.float32(0)

    def mask(hit):
        return jnp.where(hit, one, zero).astype(jnp.bfloat16)

    def start_of(zz, xx):
        return pl.multiple_of((zz * 2 + xx) * width, width)

    def times_of(zz, xx):
        return (lax.broadcasted_iota(jnp.int32, (1, width), 1) + start_of(zz, xx)) // orb

    def left_of(zz, xx, hs):
        left = []
        for t in range(cols):
            keep = mask(times_of(zz, xx) >= blocks[me] * cols + t)
            left += [g_v[h, t, :, pl.ds(start_of(zz, xx), width)] * keep for h in hs]
        return jnp.concatenate(left, axis=0)

    def right_of(zz, xx):
        right = []
        for f in range(fronts):
            keep = mask(times_of(zz, xx) <= front[f])
            right.append(jnp.concatenate([all_s[zz, xx, 0, f], all_s[zz, xx, 1, f]], axis=1) * keep)
        return jnp.concatenate(right, axis=0)

    def product(left, right):
        return lax.dot_general(left, right, (((1,), (1,)), ((), ())), preferred_element_type=jnp.float32)

    def outward(step):
        def both(d):
            @pl.when(z + d < lines)
            def _():
                step(z + d, d)

            @pl.when(z >= d)
            def _():
                step(z - d, d)

        return both

    @outward
    def z_relay(zz, d):
        with scope("Fz"):
            z_copy(zz).wait_recv()
        @pl.when((zz != special) | ~skips)
        def _():
            x_copy(zz).start()

        c_copy(zz, xi).start()

    def x_step(zz, d):
        with scope("Gx"):
            x_copy(zz).wait_recv()
        c_copy(zz, 1 - xi).start()

    x_relay = outward(x_step)

    def c_wait(zz):
        arrived(all_s.at[zz, :, 1 - core], c_recv.at[dist(zz)])

    def value(d):
        zz = xor(z, d, lines)
        lefts = [left_of(zz, xx, range(2)) for xx in range(2)]
        with scope("Hc"):
            c_wait(zz)
        return product(jnp.concatenate(lefts, axis=1), jnp.concatenate([right_of(zz, 0), right_of(zz, 1)], axis=1))

    def use(d):
        acc[...] += value(d).reshape(acc.shape)

    z_relay(1)
    with scope("Ex0"):
        x_step(z, 0)

    @pl.when(turns_in)
    def _():
        @pl.when(~direct)
        def _():
            turn_copy(0).start()

        loop(1, late, lambda zz: turn_copy(zz).start())

    loop(2, 3, z_relay)
    with scope("Eown"):
        arrived(sent.at[pl.ds(0, 2 * (s_hbm.size + g_hbm.size) // (2 * lanes))], loc.at[2])
        load_p.wait()
        load_b.wait()
        c_wait(z)
    start_rows = product(left_of(z, 0, (o,)), right_of(z, 0)) + product(left_of(z, 1, (o,)), right_of(z, 1))
    for t in range(cols):
        prev = jnp.concatenate([p_v[f, t] for f in range(fronts)], axis=1)
        p_all[o, t] = start_rows[t * half:(t + 1) * half] + prev
    p_copy.start()

    loop(3, lines, z_relay)
    x_relay(1)

    with scope("Idz"):
        @pl.when(has_rows)
        def _():
            arrived(col_d.at[pl.ds(0, late - 1)], near_recv.at[1])

        @pl.when(z < late)
        def _():
            arrived(col_d, near_recv.at[1])

    sums[0] = lax.fori_loop(1, late, lambda d, v: v + col_d[d], col_d[0])
    sums[4] = sums[0]

    @pl.when(~beside)
    def _():
        for c in sum_copies:
            c.start()

    @pl.when(~first)
    def _():
        core_sum.start()


    loop(2, lines, x_relay)

    @pl.when(first)
    def _():
        with scope("Icross"):
            arrived(cross_d, near_recv.at[3])
        sums[4] = lax.fori_loop(0, late, lambda d, v: v + cross_d[d], sums[0])
        sums[1] = jnp.zeros_like(sums[1])
        sums[2] = jnp.zeros_like(sums[2])
        core_sum.start()

    with scope("Jg"):
        far = g_hbm.size * (lines - 1) // lines + 2 * p_all.size // 2
        arrived(sent.at[pl.ds(0, 2 * far // (2 * lanes))], near_recv.at[0])
    for t in range(cols):
        for h in range(2):
            acc[t, h] = p_all[h, t]
    loop(1, lines - 1, use)

    final = value(lines - 1) + acc[...].reshape(cols * orb, fronts * orb)
    combined = [final[t * orb:(t + 1) * orb] for t in range(cols)]
    own = split(jnp.concatenate([jnp.where(o == 0, c[:half], c[half:]) for c in combined], axis=0))
    turns = split(jnp.concatenate([combined[(t + k) % cols] for k in range(fronts) for t in range(cols)], axis=0))
    with scope("Lw"):
        @pl.when(first)
        def _():
            core_sum.wait_recv()

        @pl.when(~first)
        def _():
            arrived(sums.at[pl.ds(1, 3)], near_recv.at[2])

    same, other = sums[4] + sums[1], sums[3] + sums[2]
    rows = [jnp.where(core == 0, same, other), jnp.where(core == 0, other, same)]
    mine = jnp.where(o == 0, rows[0], rows[1])
    lane = lax.broadcasted_iota(jnp.int32, (half, fronts * orb), 1) // orb
    none = jnp.zeros_like(mine)
    weight = split(jnp.concatenate([jnp.where(lane == f, r, none) for f in range(fronts) for r in rows], axis=0))
    own_weight = split(jnp.concatenate([jnp.where(lane == f, mine, none) for f in range(fronts)], axis=0))

    def times(a, b):
        return lax.dot_general(jnp.concatenate([a[0], a[1], a[0]], axis=1),
                               jnp.concatenate([b[0], b[0], b[1]], axis=1),
                               (((1,), (1,)), ((), ())), preferred_element_type=jnp.float32)

    def place(f, t):
        k = (t - f) % fronts
        return slice(k * cols * orb, (k + 1) * cols * orb)

    g_new = times(own, weight)
    flipped = times(own_weight, turns)
    for t in range(cols):
        g_t = g_new[t * half:(t + 1) * half]
        turned = sum(jnp.where(lane == f, flipped[f * half:(f + 1) * half, place(f, t)], none) for f in range(fronts))
        s_t = COUPLING * g_t * g_t * turned
        out[0, t] = g_t
        out[1, t] = s_t

    with scope("Msend"):
        @pl.when(has_rows)
        def _():
            dc_copy.wait_send()
            arrived(sent_rows, sends)

        @pl.when(turns_in)
        def _():
            @pl.when(~direct)
            def _():
                turn_copy(0).wait_send()

            arrived(all_s.at[pl.ds(0, late - 1), 0, 0], sends)

        @pl.when(across)
        def _():
            root_copy.wait_send()

        @pl.when(~skips)
        def _():
            arrived(all_s.at[0, 0, 0], sends)

        @pl.when(aside)
        def _():
            droot_copy.wait_send()

        @pl.when(~beside)
        def _():
            arrived(all_s.at[0, 0, 0], sends)

        arrived(sent, sends)


def body(lines, g_hist, sigma_hist, diag_inv, previous, block_of_slot, front_pos):
    cols, half, depth = g_hist.shape
    fronts, orb, lanes = sigma_hist.shape
    hbm = pl.BlockSpec(memory_space=pl.ANY)
    dma = pltpu.SemaphoreType.DMA
    regular = pltpu.SemaphoreType.REGULAR
    f32 = jnp.float32
    packed = (orb // 2, 2 * orb)
    width = 2 * lanes
    sent = 2 * (4 * lines - 2) * sigma_hist.size + 2 * g_hist.size * (lines - 1) // lines
    sent += 4 * orb * orb + 4 * cols * half * fronts * orb
    flops = 2 * cols * orb * depth * orb * fronts
    out = pl.pallas_call(
        functools.partial(kernel, lines),
        out_shape=pltpu.VMEM((fronts, cols, half, 2 * orb), f32),
        in_specs=[hbm] * 6,
        out_specs=pl.BlockSpec(memory_space=pltpu.VMEM),
        scratch_shapes=[
            pltpu.SMEM(block_of_slot.shape, jnp.int32),
            pltpu.SMEM(front_pos.shape, jnp.int32),
            pltpu.VMEM((2,) + g_hist.shape, g_hist.dtype),
            pltpu.VMEM((lines, 2, 2) + sigma_hist.shape, sigma_hist.dtype),
            pltpu.VMEM((2,) + diag_inv.shape, f32),
            pltpu.VMEM(previous.shape, f32),
            pltpu.VMEM((2, cols, half, fronts * orb), f32),
            pltpu.VMEM((cols, 2, half, fronts * orb), f32),
            pltpu.VMEM((lines // 2,) + packed, f32),
            pltpu.VMEM((lines // 2,) + packed, f32),
            pltpu.VMEM((5,) + packed, f32),
            pltpu.VMEM((sent // width, width // 2), jnp.bfloat16),
            pltpu.VMEM((lines - 1,) + packed, f32),
            dma((3,)), dma,
            dma((lines - 1,)), dma((lines,)), dma((lines,)),
            dma((4,)), regular((2 + lines,)),
        ],
        compiler_params=pltpu.CompilerParams(collective_id=0, has_side_effects=True),
        cost_estimate=pl.CostEstimate(flops=flops, bytes_accessed=2 * g_hist.size, transcendentals=0),
    )(block_of_slot, front_pos, g_hist, sigma_hist, diag_inv, previous)
    return tuple(jnp.stack([out[k, ..., f * orb:(f + 1) * orb] for f in range(fronts)]) for k in range(2))


def solution(mesh):
    lines = mesh.shape["hist"] // 4
    in_specs = (
        P("hist", "orb", None),
        P(None, None, "hist"),
        P("hist", None, None),
        P(None, "hist", "orb", None),
        P(),
        P(),
    )
    out_specs = (P(None, "hist", "orb", None), P(None, "hist", "orb", None))
    return jax.shard_map(functools.partial(body, lines), mesh=mesh, in_specs=in_specs,
                         out_specs=out_specs, check_vma=False)
```

```python
import functools

import jax
import jax.numpy as jnp
from jax import lax
from jax.experimental import pallas as pl
from jax.experimental.pallas import tpu as pltpu
from jax.sharding import PartitionSpec as P

COUPLING = 0.5
MESH = pl.DeviceIdType.MESH


def xor(a, b, size):
    out, bit = 0, 1
    while bit < size:
        out = out + bit * ((a // bit + b // bit) % 2)
        bit *= 2
    return out


def loop(low, high, step):
    if high - low <= 8:
        for i in range(low, high):
            step(i)
    else:
        lax.fori_loop(low, high, lambda i, c: (step(i), c)[1], 0)


def split(x):
    high = x.astype(jnp.bfloat16)
    return high, (x - high.astype(jnp.float32)).astype(jnp.bfloat16)


def kernel(lines, blocks_hbm, front_hbm, g_hbm, s_hbm, d_hbm, p_hbm, out,
           blocks, front, g_v, all_s, d_v, p_v, p_all, acc, col_d, cross_d, sums, sent, sent_rows,
           loc, sends, z_recv, x_recv, c_recv, near_recv, ready):
    cols, half = g_hbm.shape[0], g_hbm.shape[1]
    fronts, orb, lanes = s_hbm.shape
    width = 2 * lanes
    me = lax.axis_index("hist")
    o = lax.axis_index("orb")
    core = me % 2
    xi = (me // 2) % 2
    z = me // 4
    late = lines // 2
    has_rows = z >= late
    front_plane = o == 0
    first = (z == 0) & (xi == 0) & front_plane
    beside = (z == 0) & (xi == 1) & front_plane
    direct = front_plane & (core == 0)
    across = (z == lines - 1) & (xi == 1) & direct
    turns_in = (z == lines - 1) & (xi == 0)
    skips = (z < late) & (xi == 1)
    aside = has_rows & (xi == 1) & front_plane
    special = jnp.where(z == lines - 1, 0, lines - 1)

    def at(zz, xx, cc):
        return (zz * 2 + xx) * 2 + cc

    def scope(name):
        return jax.named_scope(name)

    y_peer = (me, 1 - o)
    core_peer = (at(z, xi, 1 - core), o)
    x_peer = (at(z, 1 - xi, core), o)
    xc_peer = (at(z, 1 - xi, 1 - core), o)
    near = ((y_peer, o), (core_peer, core), (x_peer, xi), (xc_peer, xi))

    def z_peer(zz):
        return (at(zz, xi, core), o)

    def dist(zz):
        return xor(zz, z, lines)

    barrier = pltpu.get_barrier_semaphore()

    def signal(sem, peer):
        pl.semaphore_signal(sem, inc=1, device_id=peer, device_id_type=MESH)

    def above(step):
        def one(zz):
            @pl.when(zz > z)
            def _():
                step(zz)

        loop(1, lines, one)

    def below(step, low=0):
        def one(zz):
            @pl.when(zz < z)
            def _():
                step(zz)

        loop(low, lines - 1, one)

    above(lambda zz: signal(barrier, z_peer(zz)))

    for peer, upper in near:
        @pl.when(upper == 0)
        def _():
            signal(barrier, peer)

    @pl.when(first)
    def _():
        loop(late, lines, lambda zz: signal(barrier, (at(zz, 1, core), o)))

    load_f = pltpu.make_async_copy(front_hbm, front, loc.at[0])
    load_d = pltpu.make_async_copy(d_hbm, d_v.at[core], loc.at[1])
    load_s = pltpu.make_async_copy(s_hbm, all_s.at[z, xi, core], loc.at[2])
    load_g = pltpu.make_async_copy(g_hbm, g_v.at[o], loc.at[2])
    load_p = pltpu.make_async_copy(p_hbm, p_v, loc.at[1])
    load_b = pltpu.make_async_copy(blocks_hbm, blocks, loc.at[0])
    load_f.start()

    @pl.when(has_rows)
    def _():
        load_d.start()

    earlier = z + 2 * xi + core + o + jnp.where(aside, 1, 0)
    with scope("Abar"):
        @pl.when(earlier > 0)
        def _():
            pl.semaphore_wait(barrier, earlier)

    def send(src, dst, rsem, peer):
        return pltpu.make_async_remote_copy(
            src_ref=src, dst_ref=dst, send_sem=sends, recv_sem=rsem,
            device_id=peer, device_id_type=MESH)

    def arrived(ref, sem):
        pltpu.make_async_copy(ref, ref, sem).wait()

    def z_copy(zz):
        return send(s_hbm, all_s.at[z, xi, core], z_recv.at[dist(zz) - 1], z_peer(zz))

    def x_copy(zz, own=False):
        ref = all_s.at[zz, xi, core]
        return send(s_hbm if own else ref, ref, x_recv.at[dist(zz)], x_peer)

    root_copy = send(s_hbm, all_s.at[z, xi, core], x_recv.at[z], (core, o))

    def turn_copy(zz):
        ref = all_s.at[lines - 1, 1, core]
        return send(ref, ref, x_recv.at[xor(zz, lines - 1, lines)], z_peer(zz))


    def c_copy(zz, xx, own=False):
        ref = all_s.at[zz, xx, core]
        return send(s_hbm if own else ref, ref, c_recv.at[dist(zz)], core_peer)

    def part_of(zz):
        return pl.ds(pl.multiple_of(zz * 2 * width, 2 * width), 2 * width)

    def g_copy(d):
        part = part_of(xor(z, d, lines))
        return send(g_hbm.at[:, :, part], g_v.at[o, :, :, part], near_recv.at[0], y_peer)

    def dz_copy(zz):
        return send(col_d.at[z - late], col_d.at[z - late], near_recv.at[1], z_peer(zz))

    droot_copy = send(col_d.at[z - late], cross_d.at[z - late], near_recv.at[3], (core, o))
    p_copy = send(p_all.at[o], p_all.at[o], near_recv.at[0], y_peer)
    dc_copy = send(d_hbm, d_v.at[core], near_recv.at[3], core_peer)
    sum_copies = [send(sums.at[0], sums.at[1 + k], near_recv.at[2], peer)
                  for k, peer in enumerate((x_peer, xc_peer))]
    core_sum = send(sums.at[4], sums.at[3], near_recv.at[2], core_peer)

    @pl.when(has_rows & (core == 1))
    def _():
        dc_copy.start()

    @pl.when(z == lines - 1)
    def _():
        z_copy(lines - 2).start()
        loop(0, lines - 2, lambda zz: z_copy(zz).start())

        @pl.when(across)
        def _():
            root_copy.start()

    @pl.when(z < lines - 1)
    def _():
        below(lambda zz: z_copy(zz).start())

    for k, (peer, upper) in enumerate(near):
        @pl.when(upper == 1)
        def _():
            signal(ready.at[min(k, 2)], peer)

    below(lambda zz: signal(ready.at[2 + dist(zz)], z_peer(zz)))

    @pl.when(xi == 1)
    def _():
        x_copy(z, True).start()

    @pl.when(core == 1)
    def _():
        c_copy(z, xi, True).start()

    @pl.when(o == 1)
    def _():
        loop(1, lines, lambda d: g_copy(d).start())

    load_s.start()
    load_g.start()

    @pl.when(core == 0)
    def _():
        with scope("Bcore"):
            pl.semaphore_wait(ready.at[1], 1)

        @pl.when(has_rows)
        def _():
            dc_copy.start()

        c_copy(z, xi, True).start()

    load_f.wait()
    load_b.start()

    @pl.when(has_rows)
    def _():
        with scope("Bload"):
            load_d.wait()
            dc_copy.wait_recv()
        rows = []
        for f in range(fronts):
            mine = front[f]
            row = d_v[(mine // cols) % 2, mine % cols, pl.ds(core * half, half)]
            rows.append(jnp.where(mine // (2 * cols) == me // 2, row, jnp.zeros_like(row)))
        col_d[z - late] = jnp.concatenate(rows, axis=1)

        @pl.when(aside)
        def _():
            droot_copy.start()

        below(lambda zz: dz_copy(zz).start())

    load_p.start()
    with scope("Cnear"):
        @pl.when(o == 0)
        def _():
            pl.semaphore_wait(ready.at[0], 1)
            loop(1, lines, lambda d: g_copy(d).start())

        @pl.when(xi == 0)
        def _():
            pl.semaphore_wait(ready.at[2], 2)
            x_copy(z, True).start()

    def depart(zz):
        pl.semaphore_wait(ready.at[2 + dist(zz)], 1)
        z_copy(zz).start()

        @pl.when(has_rows)
        def _():
            dz_copy(zz).start()

    with scope("Dfar"):
        above(depart)

    one, zero = jnp.float32(1), jnp.float32(0)

    def mask(hit):
        return jnp.where(hit, one, zero).astype(jnp.bfloat16)

    def start_of(zz, xx):
        return pl.multiple_of((zz * 2 + xx) * width, width)

    def times_of(zz, xx):
        return (lax.broadcasted_iota(jnp.int32, (1, width), 1) + start_of(zz, xx)) // orb

    def left_of(zz, xx, hs):
        left = []
        for t in range(cols):
            keep = mask(times_of(zz, xx) >= blocks[me] * cols + t)
            left += [g_v[h, t, :, pl.ds(start_of(zz, xx), width)] * keep for h in hs]
        return jnp.concatenate(left, axis=0)

    def right_of(zz, xx):
        right = []
        for f in range(fronts):
            keep = mask(times_of(zz, xx) <= front[f])
            right.append(jnp.concatenate([all_s[zz, xx, 0, f], all_s[zz, xx, 1, f]], axis=1) * keep)
        return jnp.concatenate(right, axis=0)

    def product(left, right):
        return lax.dot_general(left, right, (((1,), (1,)), ((), ())), preferred_element_type=jnp.float32)

    def outward(step):
        def both(d):
            @pl.when(z + d < lines)
            def _():
                step(z + d, d)

            @pl.when(z >= d)
            def _():
                step(z - d, d)

        return both

    @outward
    def z_relay(zz, d):
        with scope("Fz"):
            z_copy(zz).wait_recv()
        @pl.when((zz != special) | ~skips)
        def _():
            x_copy(zz).start()

        c_copy(zz, xi).start()

    def x_step(zz, d):
        with scope("Gx"):
            x_copy(zz).wait_recv()
        c_copy(zz, 1 - xi).start()

    x_relay = outward(x_step)

    def c_wait(zz):
        arrived(all_s.at[zz, :, 1 - core], c_recv.at[dist(zz)])

    def value(d):
        zz = xor(z, d, lines)
        lefts = [left_of(zz, xx, range(2)) for xx in range(2)]
        with scope("Hc"):
            c_wait(zz)
        return product(jnp.concatenate(lefts, axis=1), jnp.concatenate([right_of(zz, 0), right_of(zz, 1)], axis=1))

    def use(d):
        acc[...] += value(d).reshape(acc.shape)

    z_relay(1)
    with scope("Ex0"):
        x_step(z, 0)

    @pl.when(turns_in)
    def _():
        @pl.when(~direct)
        def _():
            turn_copy(0).start()

        loop(1, late, lambda zz: turn_copy(zz).start())

    loop(2, 3, z_relay)
    with scope("Eown"):
        arrived(sent.at[pl.ds(0, 2 * (s_hbm.size + g_hbm.size) // (2 * lanes))], loc.at[2])
        load_p.wait()
        load_b.wait()
        c_wait(z)
    start_rows = product(left_of(z, 0, (o,)), right_of(z, 0)) + product(left_of(z, 1, (o,)), right_of(z, 1))
    for t in range(cols):
        prev = jnp.concatenate([p_v[f, t] for f in range(fronts)], axis=1)
        p_all[o, t] = start_rows[t * half:(t + 1) * half] + prev
    p_copy.start()

    loop(3, lines, z_relay)
    def reduce_rows():
        with scope("Idz"):
            @pl.when(has_rows)
            def _():
                arrived(col_d.at[pl.ds(0, late - 1)], near_recv.at[1])

            @pl.when(z < late)
            def _():
                arrived(col_d, near_recv.at[1])

        sums[0] = lax.fori_loop(1, late, lambda d, v: v + col_d[d], col_d[0])
        sums[4] = sums[0]

        @pl.when(~beside)
        def _():
            for c in sum_copies:
                c.start()

        @pl.when(~first)
        def _():
            core_sum.start()

    @pl.when(has_rows)
    def _():
        reduce_rows()

    x_relay(1)

    @pl.when(~has_rows)
    def _():
        reduce_rows()


    loop(2, lines, x_relay)

    @pl.when(first)
    def _():
        with scope("Icross"):
            arrived(cross_d, near_recv.at[3])
        sums[4] = lax.fori_loop(0, late, lambda d, v: v + cross_d[d], sums[0])
        sums[1] = jnp.zeros_like(sums[1])
        sums[2] = jnp.zeros_like(sums[2])
        core_sum.start()

    with scope("Jg"):
        far = g_hbm.size * (lines - 1) // lines + 2 * p_all.size // 2
        arrived(sent.at[pl.ds(0, 2 * far // (2 * lanes))], near_recv.at[0])
    for t in range(cols):
        for h in range(2):
            acc[t, h] = p_all[h, t]
    loop(1, lines - 1, use)

    final = value(lines - 1) + acc[...].reshape(cols * orb, fronts * orb)
    combined = [final[t * orb:(t + 1) * orb] for t in range(cols)]
    own = split(jnp.concatenate([jnp.where(o == 0, c[:half], c[half:]) for c in combined], axis=0))
    turns = split(jnp.concatenate([combined[(t + k) % cols] for k in range(fronts) for t in range(cols)], axis=0))
    with scope("Lw"):
        @pl.when(first)
        def _():
            core_sum.wait_recv()

        @pl.when(~first)
        def _():
            arrived(sums.at[pl.ds(1, 3)], near_recv.at[2])

    same, other = sums[4] + sums[1], sums[3] + sums[2]
    rows = [jnp.where(core == 0, same, other), jnp.where(core == 0, other, same)]
    mine = jnp.where(o == 0, rows[0], rows[1])
    lane = lax.broadcasted_iota(jnp.int32, (half, fronts * orb), 1) // orb
    none = jnp.zeros_like(mine)
    weight = split(jnp.concatenate([jnp.where(lane == f, r, none) for f in range(fronts) for r in rows], axis=0))
    own_weight = split(jnp.concatenate([jnp.where(lane == f, mine, none) for f in range(fronts)], axis=0))

    def times(a, b):
        return lax.dot_general(jnp.concatenate([a[0], a[1], a[0]], axis=1),
                               jnp.concatenate([b[0], b[0], b[1]], axis=1),
                               (((1,), (1,)), ((), ())), preferred_element_type=jnp.float32)

    def place(f, t):
        k = (t - f) % fronts
        return slice(k * cols * orb, (k + 1) * cols * orb)

    g_new = times(own, weight)
    flipped = times(own_weight, turns)
    for t in range(cols):
        g_t = g_new[t * half:(t + 1) * half]
        turned = sum(jnp.where(lane == f, flipped[f * half:(f + 1) * half, place(f, t)], none) for f in range(fronts))
        s_t = COUPLING * g_t * g_t * turned
        out[0, t] = g_t
        out[1, t] = s_t

    with scope("Msend"):
        @pl.when(has_rows)
        def _():
            dc_copy.wait_send()
            arrived(sent_rows, sends)

        @pl.when(turns_in)
        def _():
            @pl.when(~direct)
            def _():
                turn_copy(0).wait_send()

            arrived(all_s.at[pl.ds(0, late - 1), 0, 0], sends)

        @pl.when(across)
        def _():
            root_copy.wait_send()

        @pl.when(~skips)
        def _():
            arrived(all_s.at[0, 0, 0], sends)

        @pl.when(aside)
        def _():
            droot_copy.wait_send()

        @pl.when(~beside)
        def _():
            arrived(all_s.at[0, 0, 0], sends)

        arrived(sent, sends)


def body(lines, g_hist, sigma_hist, diag_inv, previous, block_of_slot, front_pos):
    cols, half, depth = g_hist.shape
    fronts, orb, lanes = sigma_hist.shape
    hbm = pl.BlockSpec(memory_space=pl.ANY)
    dma = pltpu.SemaphoreType.DMA
    regular = pltpu.SemaphoreType.REGULAR
    f32 = jnp.float32
    packed = (orb // 2, 2 * orb)
    width = 2 * lanes
    sent = 2 * (4 * lines - 2) * sigma_hist.size + 2 * g_hist.size * (lines - 1) // lines
    sent += 4 * orb * orb + 4 * cols * half * fronts * orb
    flops = 2 * cols * orb * depth * orb * fronts
    out = pl.pallas_call(
        functools.partial(kernel, lines),
        out_shape=pltpu.VMEM((fronts, cols, half, 2 * orb), f32),
        in_specs=[hbm] * 6,
        out_specs=pl.BlockSpec(memory_space=pltpu.VMEM),
        scratch_shapes=[
            pltpu.SMEM(block_of_slot.shape, jnp.int32),
            pltpu.SMEM(front_pos.shape, jnp.int32),
            pltpu.VMEM((2,) + g_hist.shape, g_hist.dtype),
            pltpu.VMEM((lines, 2, 2) + sigma_hist.shape, sigma_hist.dtype),
            pltpu.VMEM((2,) + diag_inv.shape, f32),
            pltpu.VMEM(previous.shape, f32),
            pltpu.VMEM((2, cols, half, fronts * orb), f32),
            pltpu.VMEM((cols, 2, half, fronts * orb), f32),
            pltpu.VMEM((lines // 2,) + packed, f32),
            pltpu.VMEM((lines // 2,) + packed, f32),
            pltpu.VMEM((5,) + packed, f32),
            pltpu.VMEM((sent // width, width // 2), jnp.bfloat16),
            pltpu.VMEM((lines - 1,) + packed, f32),
            dma((3,)), dma,
            dma((lines - 1,)), dma((lines,)), dma((lines,)),
            dma((4,)), regular((2 + lines,)),
        ],
        compiler_params=pltpu.CompilerParams(collective_id=0, has_side_effects=True),
        cost_estimate=pl.CostEstimate(flops=flops, bytes_accessed=2 * g_hist.size, transcendentals=0),
    )(block_of_slot, front_pos, g_hist, sigma_hist, diag_inv, previous)
    return tuple(jnp.stack([out[k, ..., f * orb:(f + 1) * orb] for f in range(fronts)]) for k in range(2))


def solution(mesh):
    lines = mesh.shape["hist"] // 4
    in_specs = (
        P("hist", "orb", None),
        P(None, None, "hist"),
        P("hist", None, None),
        P(None, "hist", "orb", None),
        P(),
        P(),
    )
    out_specs = (P(None, "hist", "orb", None), P(None, "hist", "orb", None))
    return jax.shard_map(functools.partial(body, lines), mesh=mesh, in_specs=in_specs,
                         out_specs=out_specs, check_vma=False)
```

```python
import functools

import jax
import jax.numpy as jnp
from jax import lax
from jax.experimental import pallas as pl
from jax.experimental.pallas import tpu as pltpu
from jax.sharding import PartitionSpec as P

COUPLING = 0.5
MESH = pl.DeviceIdType.MESH


def xor(a, b, size):
    out, bit = 0, 1
    while bit < size:
        out = out + bit * ((a // bit + b // bit) % 2)
        bit *= 2
    return out


def loop(low, high, step):
    if high - low <= 8:
        for i in range(low, high):
            step(i)
    else:
        lax.fori_loop(low, high, lambda i, c: (step(i), c)[1], 0)


def split(x):
    high = x.astype(jnp.bfloat16)
    return high, (x - high.astype(jnp.float32)).astype(jnp.bfloat16)


def kernel(lines, blocks_hbm, front_hbm, g_hbm, s_hbm, d_hbm, p_hbm, out,
           blocks, front, g_v, all_s, d_v, p_v, p_all, acc, col_d, cross_d, sums, sent, sent_rows,
           loc, sends, z_recv, x_recv, c_recv, near_recv, ready):
    cols, half = g_hbm.shape[0], g_hbm.shape[1]
    fronts, orb, lanes = s_hbm.shape
    width = 2 * lanes
    me = lax.axis_index("hist")
    o = lax.axis_index("orb")
    core = me % 2
    xi = (me // 2) % 2
    z = me // 4
    late = lines // 2
    has_rows = z >= late
    front_plane = o == 0
    first = (z == 0) & (xi == 0) & front_plane
    beside = (z == 0) & (xi == 1) & front_plane
    direct = front_plane & (core == 0)
    across = (z == lines - 1) & (xi == 1) & direct
    turns_in = (z == lines - 1) & (xi == 0)
    skips = (z < late) & (xi == 1)
    aside = has_rows & (xi == 1) & front_plane
    special = jnp.where(z == lines - 1, 0, lines - 1)

    def at(zz, xx, cc):
        return (zz * 2 + xx) * 2 + cc

    def scope(name):
        return jax.named_scope(name)

    y_peer = (me, 1 - o)
    core_peer = (at(z, xi, 1 - core), o)
    x_peer = (at(z, 1 - xi, core), o)
    xc_peer = (at(z, 1 - xi, 1 - core), o)
    near = ((y_peer, o), (core_peer, core), (x_peer, xi), (xc_peer, xi))

    def z_peer(zz):
        return (at(zz, xi, core), o)

    def dist(zz):
        return xor(zz, z, lines)

    barrier = pltpu.get_barrier_semaphore()

    def signal(sem, peer):
        pl.semaphore_signal(sem, inc=1, device_id=peer, device_id_type=MESH)

    def above(step):
        def one(zz):
            @pl.when(zz > z)
            def _():
                step(zz)

        loop(1, lines, one)

    def below(step, low=0):
        def one(zz):
            @pl.when(zz < z)
            def _():
                step(zz)

        loop(low, lines - 1, one)

    above(lambda zz: signal(barrier, z_peer(zz)))

    for peer, upper in near:
        @pl.when(upper == 0)
        def _():
            signal(barrier, peer)

    @pl.when(first)
    def _():
        loop(late, lines, lambda zz: signal(barrier, (at(zz, 1, core), o)))

    load_f = pltpu.make_async_copy(front_hbm, front, loc.at[0])
    load_d = pltpu.make_async_copy(d_hbm, d_v.at[core], loc.at[1])
    load_s = pltpu.make_async_copy(s_hbm, all_s.at[z, xi, core], loc.at[2])
    load_g = pltpu.make_async_copy(g_hbm, g_v.at[o], loc.at[2])
    load_p = pltpu.make_async_copy(p_hbm, p_v, loc.at[1])
    load_b = pltpu.make_async_copy(blocks_hbm, blocks, loc.at[0])
    load_f.start()

    @pl.when(has_rows)
    def _():
        load_d.start()

    earlier = z + 2 * xi + core + o + jnp.where(aside, 1, 0)
    with scope("Abar"):
        @pl.when(earlier > 0)
        def _():
            pl.semaphore_wait(barrier, earlier)

    def send(src, dst, rsem, peer):
        return pltpu.make_async_remote_copy(
            src_ref=src, dst_ref=dst, send_sem=sends, recv_sem=rsem,
            device_id=peer, device_id_type=MESH)

    def arrived(ref, sem):
        pltpu.make_async_copy(ref, ref, sem).wait()

    def z_copy(zz):
        return send(s_hbm, all_s.at[z, xi, core], z_recv.at[dist(zz) - 1], z_peer(zz))

    def x_copy(zz, own=False):
        ref = all_s.at[zz, xi, core]
        return send(s_hbm if own else ref, ref, x_recv.at[dist(zz)], x_peer)

    root_copy = send(s_hbm, all_s.at[z, xi, core], x_recv.at[z], (core, o))

    def turn_copy(zz):
        ref = all_s.at[lines - 1, 1, core]
        return send(ref, ref, x_recv.at[xor(zz, lines - 1, lines)], z_peer(zz))


    def c_copy(zz, xx, own=False):
        ref = all_s.at[zz, xx, core]
        return send(s_hbm if own else ref, ref, c_recv.at[dist(zz)], core_peer)

    def part_of(zz):
        return pl.ds(pl.multiple_of(zz * 2 * width, 2 * width), 2 * width)

    def g_copy(d):
        part = part_of(xor(z, d, lines))
        return send(g_hbm.at[:, :, part], g_v.at[o, :, :, part], near_recv.at[0], y_peer)

    def dz_copy(zz):
        return send(col_d.at[z - late], col_d.at[z - late], near_recv.at[1], z_peer(zz))

    droot_copy = send(col_d.at[z - late], cross_d.at[z - late], near_recv.at[3], (core, o))
    p_copy = send(p_all.at[o], p_all.at[o], near_recv.at[0], y_peer)
    dc_copy = send(d_hbm, d_v.at[core], near_recv.at[3], core_peer)
    sum_copies = [send(sums.at[0], sums.at[1 + k], near_recv.at[2], peer)
                  for k, peer in enumerate((x_peer, xc_peer))]
    core_sum = send(sums.at[4], sums.at[3], near_recv.at[2], core_peer)

    @pl.when(has_rows & (core == 1))
    def _():
        dc_copy.start()

    @pl.when(z == lines - 1)
    def _():
        z_copy(lines - 2).start()
        loop(0, lines - 2, lambda zz: z_copy(zz).start())

        @pl.when(across)
        def _():
            root_copy.start()

    @pl.when(z < lines - 1)
    def _():
        below(lambda zz: z_copy(zz).start())

    for k, (peer, upper) in enumerate(near):
        @pl.when(upper == 1)
        def _():
            signal(ready.at[min(k, 2)], peer)

    below(lambda zz: signal(ready.at[2 + dist(zz)], z_peer(zz)))

    @pl.when(xi == 1)
    def _():
        x_copy(z, True).start()

    @pl.when(core == 1)
    def _():
        c_copy(z, xi, True).start()

    @pl.when(o == 1)
    def _():
        loop(1, lines, lambda d: g_copy(d).start())

    load_s.start()
    load_g.start()

    @pl.when(core == 0)
    def _():
        with scope("Bcore"):
            pl.semaphore_wait(ready.at[1], 1)

        @pl.when(has_rows)
        def _():
            dc_copy.start()

        c_copy(z, xi, True).start()

    load_f.wait()
    load_b.start()

    @pl.when(has_rows)
    def _():
        with scope("Bload"):
            load_d.wait()
            dc_copy.wait_recv()
        rows = []
        for f in range(fronts):
            mine = front[f]
            row = d_v[(mine // cols) % 2, mine % cols, pl.ds(core * half, half)]
            rows.append(jnp.where(mine // (2 * cols) == me // 2, row, jnp.zeros_like(row)))
        col_d[z - late] = jnp.concatenate(rows, axis=1)

        @pl.when(aside)
        def _():
            droot_copy.start()

        below(lambda zz: dz_copy(zz).start())

    load_p.start()
    with scope("Cnear"):
        @pl.when(o == 0)
        def _():
            pl.semaphore_wait(ready.at[0], 1)
            loop(1, lines, lambda d: g_copy(d).start())

        @pl.when(xi == 0)
        def _():
            pl.semaphore_wait(ready.at[2], 2)
            x_copy(z, True).start()

    def depart(zz):
        pl.semaphore_wait(ready.at[2 + dist(zz)], 1)
        @pl.when(has_rows)
        def _():
            dz_copy(zz).start()

        z_copy(zz).start()

    with scope("Dfar"):
        above(depart)

    one, zero = jnp.float32(1), jnp.float32(0)

    def mask(hit):
        return jnp.where(hit, one, zero).astype(jnp.bfloat16)

    def start_of(zz, xx):
        return pl.multiple_of((zz * 2 + xx) * width, width)

    def times_of(zz, xx):
        return (lax.broadcasted_iota(jnp.int32, (1, width), 1) + start_of(zz, xx)) // orb

    def left_of(zz, xx, hs):
        left = []
        for t in range(cols):
            keep = mask(times_of(zz, xx) >= blocks[me] * cols + t)
            left += [g_v[h, t, :, pl.ds(start_of(zz, xx), width)] * keep for h in hs]
        return jnp.concatenate(left, axis=0)

    def right_of(zz, xx):
        right = []
        for f in range(fronts):
            keep = mask(times_of(zz, xx) <= front[f])
            right.append(jnp.concatenate([all_s[zz, xx, 0, f], all_s[zz, xx, 1, f]], axis=1) * keep)
        return jnp.concatenate(right, axis=0)

    def product(left, right):
        return lax.dot_general(left, right, (((1,), (1,)), ((), ())), preferred_element_type=jnp.float32)

    def outward(step):
        def both(d):
            @pl.when(z + d < lines)
            def _():
                step(z + d, d)

            @pl.when(z >= d)
            def _():
                step(z - d, d)

        return both

    @outward
    def z_relay(zz, d):
        with scope("Fz"):
            z_copy(zz).wait_recv()
        c_copy(zz, xi).start()

        @pl.when((zz != special) | ~skips)
        def _():
            x_copy(zz).start()

    def x_step(zz, d):
        with scope("Gx"):
            x_copy(zz).wait_recv()
        c_copy(zz, 1 - xi).start()

    x_relay = outward(x_step)

    def c_wait(zz):
        arrived(all_s.at[zz, :, 1 - core], c_recv.at[dist(zz)])

    def value(d):
        zz = xor(z, d, lines)
        lefts = [left_of(zz, xx, range(2)) for xx in range(2)]
        with scope("Hc"):
            c_wait(zz)
        return product(jnp.concatenate(lefts, axis=1), jnp.concatenate([right_of(zz, 0), right_of(zz, 1)], axis=1))

    def use(d):
        acc[...] += value(d).reshape(acc.shape)

    z_relay(1)
    with scope("Ex0"):
        x_step(z, 0)

    @pl.when(turns_in)
    def _():
        @pl.when(~direct)
        def _():
            turn_copy(0).start()

        loop(1, late, lambda zz: turn_copy(zz).start())

    loop(2, 3, z_relay)
    with scope("Eown"):
        arrived(sent.at[pl.ds(0, 2 * (s_hbm.size + g_hbm.size) // (2 * lanes))], loc.at[2])
        load_p.wait()
        load_b.wait()
        c_wait(z)
    start_rows = product(left_of(z, 0, (o,)), right_of(z, 0)) + product(left_of(z, 1, (o,)), right_of(z, 1))
    for t in range(cols):
        prev = jnp.concatenate([p_v[f, t] for f in range(fronts)], axis=1)
        p_all[o, t] = start_rows[t * half:(t + 1) * half] + prev
    p_copy.start()

    loop(3, lines, z_relay)
    def reduce_rows():
        with scope("Idz"):
            @pl.when(has_rows)
            def _():
                arrived(col_d.at[pl.ds(0, late - 1)], near_recv.at[1])

            @pl.when(z < late)
            def _():
                arrived(col_d, near_recv.at[1])

        sums[0] = lax.fori_loop(1, late, lambda d, v: v + col_d[d], col_d[0])
        sums[4] = sums[0]

        @pl.when(~beside)
        def _():
            for c in sum_copies:
                c.start()

        @pl.when(~first)
        def _():
            core_sum.start()

    @pl.when(has_rows)
    def _():
        reduce_rows()

    x_relay(1)

    @pl.when(~has_rows)
    def _():
        reduce_rows()


    loop(2, lines, x_relay)

    @pl.when(first)
    def _():
        with scope("Icross"):
            arrived(cross_d, near_recv.at[3])
        sums[4] = lax.fori_loop(0, late, lambda d, v: v + cross_d[d], sums[0])
        sums[1] = jnp.zeros_like(sums[1])
        sums[2] = jnp.zeros_like(sums[2])
        core_sum.start()

    with scope("Jg"):
        far = g_hbm.size * (lines - 1) // lines + 2 * p_all.size // 2
        arrived(sent.at[pl.ds(0, 2 * far // (2 * lanes))], near_recv.at[0])
    for t in range(cols):
        for h in range(2):
            acc[t, h] = p_all[h, t]
    loop(1, lines - 1, use)

    final = value(lines - 1) + acc[...].reshape(cols * orb, fronts * orb)
    combined = [final[t * orb:(t + 1) * orb] for t in range(cols)]
    own = split(jnp.concatenate([jnp.where(o == 0, c[:half], c[half:]) for c in combined], axis=0))
    turns = split(jnp.concatenate([combined[(t + k) % cols] for k in range(fronts) for t in range(cols)], axis=0))
    with scope("Lw"):
        @pl.when(first)
        def _():
            core_sum.wait_recv()

        @pl.when(~first)
        def _():
            arrived(sums.at[pl.ds(1, 3)], near_recv.at[2])

    same, other = sums[4] + sums[1], sums[3] + sums[2]
    rows = [jnp.where(core == 0, same, other), jnp.where(core == 0, other, same)]
    mine = jnp.where(o == 0, rows[0], rows[1])
    lane = lax.broadcasted_iota(jnp.int32, (half, fronts * orb), 1) // orb
    none = jnp.zeros_like(mine)
    weight = split(jnp.concatenate([jnp.where(lane == f, r, none) for f in range(fronts) for r in rows], axis=0))
    own_weight = split(jnp.concatenate([jnp.where(lane == f, mine, none) for f in range(fronts)], axis=0))

    def times(a, b):
        return lax.dot_general(jnp.concatenate([a[0], a[1], a[0]], axis=1),
                               jnp.concatenate([b[0], b[0], b[1]], axis=1),
                               (((1,), (1,)), ((), ())), preferred_element_type=jnp.float32)

    def place(f, t):
        k = (t - f) % fronts
        return slice(k * cols * orb, (k + 1) * cols * orb)

    g_new = times(own, weight)
    flipped = times(own_weight, turns)
    for t in range(cols):
        g_t = g_new[t * half:(t + 1) * half]
        turned = sum(jnp.where(lane == f, flipped[f * half:(f + 1) * half, place(f, t)], none) for f in range(fronts))
        s_t = COUPLING * g_t * g_t * turned
        out[0, t] = g_t
        out[1, t] = s_t

    with scope("Msend"):
        @pl.when(has_rows)
        def _():
            dc_copy.wait_send()
            arrived(sent_rows, sends)

        @pl.when(turns_in)
        def _():
            @pl.when(~direct)
            def _():
                turn_copy(0).wait_send()

            arrived(all_s.at[pl.ds(0, late - 1), 0, 0], sends)

        @pl.when(across)
        def _():
            root_copy.wait_send()

        @pl.when(~skips)
        def _():
            arrived(all_s.at[0, 0, 0], sends)

        @pl.when(aside)
        def _():
            droot_copy.wait_send()

        @pl.when(~beside)
        def _():
            arrived(all_s.at[0, 0, 0], sends)

        arrived(sent, sends)


def body(lines, g_hist, sigma_hist, diag_inv, previous, block_of_slot, front_pos):
    cols, half, depth = g_hist.shape
    fronts, orb, lanes = sigma_hist.shape
    hbm = pl.BlockSpec(memory_space=pl.ANY)
    dma = pltpu.SemaphoreType.DMA
    regular = pltpu.SemaphoreType.REGULAR
    f32 = jnp.float32
    packed = (orb // 2, 2 * orb)
    width = 2 * lanes
    sent = 2 * (4 * lines - 2) * sigma_hist.size + 2 * g_hist.size * (lines - 1) // lines
    sent += 4 * orb * orb + 4 * cols * half * fronts * orb
    flops = 2 * cols * orb * depth * orb * fronts
    out = pl.pallas_call(
        functools.partial(kernel, lines),
        out_shape=pltpu.VMEM((fronts, cols, half, 2 * orb), f32),
        in_specs=[hbm] * 6,
        out_specs=pl.BlockSpec(memory_space=pltpu.VMEM),
        scratch_shapes=[
            pltpu.SMEM(block_of_slot.shape, jnp.int32),
            pltpu.SMEM(front_pos.shape, jnp.int32),
            pltpu.VMEM((2,) + g_hist.shape, g_hist.dtype),
            pltpu.VMEM((lines, 2, 2) + sigma_hist.shape, sigma_hist.dtype),
            pltpu.VMEM((2,) + diag_inv.shape, f32),
            pltpu.VMEM(previous.shape, f32),
            pltpu.VMEM((2, cols, half, fronts * orb), f32),
            pltpu.VMEM((cols, 2, half, fronts * orb), f32),
            pltpu.VMEM((lines // 2,) + packed, f32),
            pltpu.VMEM((lines // 2,) + packed, f32),
            pltpu.VMEM((5,) + packed, f32),
            pltpu.VMEM((sent // width, width // 2), jnp.bfloat16),
            pltpu.VMEM((lines - 1,) + packed, f32),
            dma((3,)), dma,
            dma((lines - 1,)), dma((lines,)), dma((lines,)),
            dma((4,)), regular((2 + lines,)),
        ],
        compiler_params=pltpu.CompilerParams(collective_id=0, has_side_effects=True),
        cost_estimate=pl.CostEstimate(flops=flops, bytes_accessed=2 * g_hist.size, transcendentals=0),
    )(block_of_slot, front_pos, g_hist, sigma_hist, diag_inv, previous)
    return tuple(jnp.stack([out[k, ..., f * orb:(f + 1) * orb] for f in range(fronts)]) for k in range(2))


def solution(mesh):
    lines = mesh.shape["hist"] // 4
    in_specs = (
        P("hist", "orb", None),
        P(None, None, "hist"),
        P("hist", None, None),
        P(None, "hist", "orb", None),
        P(),
        P(),
    )
    out_specs = (P(None, "hist", "orb", None), P(None, "hist", "orb", None))
    return jax.shard_map(functools.partial(body, lines), mesh=mesh, in_specs=in_specs,
                         out_specs=out_specs, check_vma=False)
```
